32 devices in a mesh: gx: 4 (over x, core), gy: 2 (over y), gz: 4 (over z).
Axes of the slice: x: 2, y: 2, z: 4, core: 2. Of those that a mesh axis runs over, the one named last changes fastest.
Arguments:
- displace: float32 [3, 8, 16, 512], P(None, 'gx', 'gy', 'gz'), may hold values from -0.15 to 0.15
- occupied: int32 [8, 16, 512], P('gx', 'gy', 'gz'), may hold values from 0 to 1, as said below
- strength: float32 [8, 16, 512], P('gx', 'gy', 'gz'), may hold values from 0.5 to 2
Outputs:
- force: float32 [3, 8, 16, 512], P(None, 'gx', 'gy', 'gz')
- energy: float32 [8, 16, 512], P('gx', 'gy', 'gz')
The draws below stay inside these ranges and needn't reach their ends.
Inputs may be any that keep to these rules, and one draw needn't show every extreme that they name: `occupied`: 0 for a vacancy, 1 for an atom; the share of vacancies differs from domain to domain.
All inputs are finite; a program needn't handle non-finite values.
Results may differ from the reference program's by a relative error of at most 0.00017.
Values sent between devices are 32-bit elements; how exact they have to be, the bound alone decides.
A program may use at most 64 MiB of HBM per device.

```python
import math
import jax
import jax.numpy as jnp
from jax import lax

CX = 2
CY = 8
CZ = 128
ITERS = 3
NX = 8
NY = 16
NZ = 512


def draw_occupied(key, part):
    rate_key, site_key = jax.random.split(jax.random.fold_in(key, 17))
    domains = jax.random.randint(rate_key, (NX // CX, NY // CY, NZ // CZ), 50, 96)
    domain_rate = jnp.repeat(jnp.repeat(jnp.repeat(domains, CX, axis=0), CY, axis=1), CZ, axis=2)
    dice_rolls = jax.random.randint(site_key, (NX, NY, NZ), 0, 100)
    return (dice_rolls < domain_rate).astype(jnp.int32)


def shard_levels(stream_key, extent, cuts, low, high):
    def one(axis_at, blocks):
        heights = jax.random.uniform(jax.random.fold_in(jax.random.fold_in(stream_key, 6), axis_at), (blocks,), jnp.float32, low / len(cuts), high / len(cuts))
        return jnp.repeat(jnp.exp(heights), extent[axis_at] // blocks).reshape((-1,) + (1,) * (len(extent) - axis_at - 1))

    factor_of = one(*cuts[0])
    for cut in cuts[1:]:
        factor_of = factor_of * one(*cut)
    return factor_of


def noise(own_key, shape, width, most, cuts=(), kind=jnp.bfloat16):
    values = jax.random.normal(own_key, shape, jnp.float32) * width
    if len(cuts) > 0:
        values = shard_levels(own_key, shape, cuts, -0.22, 0.18) * values
    return jnp.clip(values, min=-most, max=most).astype(kind)


def setup_inputs(seed: int = 0) -> dict:
    seeds = jax.random.split(jax.random.key(seed), 4)
    displace = noise(seeds[0], (3, NX, NY, NZ), 0.05, 0.15, ((1, 4), (2, 2), (3, 4)), jnp.float32)
    occupied = draw_occupied(jax.random.fold_in(seeds[3], 71), 0)
    strength = jnp.clip(jnp.exp(math.log(2.0) - 1.3862944 * jax.random.uniform(seeds[2], (NX, NY, NZ), jnp.float32) ** shard_levels(seeds[2], (NX, NY, NZ), ((0, 4), (1, 2), (2, 4)), -0.2, 0.2)), 0.5, 2.0)
    return dict(displace=displace, occupied=occupied, strength=strength)


RADIUS_SQ = 4.84
STEP = 0.02

def cutoff(distance):
    inside = 1.0 - distance * distance / RADIUS_SQ
    return inside * inside

def cutoff_slope(distance):
    inside = 1.0 - distance * distance / RADIUS_SQ
    return -4.0 * inside * distance / RADIUS_SQ

def density(distance):
    return jnp.exp(-2.0 * (distance - 1.0)) * cutoff(distance)

def density_slope(distance):
    growth = jnp.exp(-2.0 * (distance - 1.0))
    return growth * (cutoff_slope(distance) - 2.0 * cutoff(distance))

def repulse(distance):
    return 0.5 * jnp.exp(-4.0 * (distance - 1.0)) * cutoff(distance)

def repulse_slope(distance):
    growth = 0.5 * jnp.exp(-4.0 * (distance - 1.0))
    return growth * (cutoff_slope(distance) - 4.0 * cutoff(distance))
FULL_OFFSETS = [(first, second, third) for first in (-1, 0, 1) for second in (-1, 0, 1) for third in (-1, 0, 1) if (first, second, third) != (0, 0, 0)]

def neighbour(padded, offset):
    return padded[..., 1 + offset[0]:1 + offset[0] + NX, 1 + offset[1]:1 + offset[1] + NY, 1 + offset[2]:1 + offset[2] + NZ]

def evaluate(displace, occupancy, weight):
    pad_disp = jnp.pad(displace, ((0, 0), (1, 1), (1, 1), (1, 1)))
    pad_weight = jnp.pad(weight, 1)

    def geometry(offset):
        lattice = jnp.array(offset, jnp.float32).reshape(3, 1, 1, 1)
        separation = lattice + neighbour(pad_disp, offset) - displace
        distance = jnp.sqrt(lax.optimization_barrier(jnp.sum(separation * separation, axis=0)))
        return (separation, distance)
    density_sum = jnp.zeros(weight.shape, jnp.float32)
    for offset in FULL_OFFSETS:
        separation, distance = geometry(offset)
        density_sum = density_sum + neighbour(pad_weight, offset) * density(distance)
    slope = occupancy * -0.5 / jnp.sqrt(1.0 + density_sum)
    pad_slope = jnp.pad(slope, 1)
    force = jnp.zeros(displace.shape, jnp.float32)
    pair_sum = jnp.zeros(weight.shape, jnp.float32)
    for offset in FULL_OFFSETS:
        separation, distance = geometry(offset)
        near_weight = neighbour(pad_weight, offset)
        near_slope = neighbour(pad_slope, offset)
        coupling = (slope * near_weight + near_slope * weight) * density_slope(distance) + weight * near_weight * repulse_slope(distance)
        force = force + coupling / distance * separation
        pair_sum = pair_sum + near_weight * repulse(distance)
    energy = occupancy * -jnp.sqrt(1.0 + density_sum) + 0.5 * weight * pair_sum
    return (force, energy)

def reference(displace, occupied, strength):
    occupancy = occupied.astype(jnp.float32)
    weight = occupancy * strength
    current = displace
    force, energy = evaluate(current, occupancy, weight)
    for step in range(ITERS - 1):
        current = current + STEP * force
        force, energy = evaluate(current, occupancy, weight)
    return (force, energy)
```

```python
import functools
import math

import jax
import jax.numpy as jnp
from jax import lax
from jax.experimental import pallas as pl
from jax.experimental.pallas import tpu as pltpu
from jax.sharding import PartitionSpec as P

ITERS = 3
RADIUS_SQ = 4.84
STEP = 0.02
AXES = ("gx", "gy", "gz")
MESH = pl.DeviceIdType.MESH
LANES = 128
DEEP = 2 * ITERS
PLANE = [(dx, dy) for dx in (-1, 0, 1) for dy in (-1, 0, 1)]
FLAT = sorted(((dx, dy, 0) for dx, dy in PLANE if (dx, dy) != (0, 0)),
              key=lambda o: (-sum(abs(a) for a in o), o))
TALL = sorted(((dx, dy, dz) for dx, dy in PLANE for dz in (-1, 1)),
              key=lambda o: (-sum(abs(a) for a in o), o))
PANELS = TALL + FLAT

RADIUS = math.sqrt(RADIUS_SQ)
UNIT = 1.0 / RADIUS
RATE = -2.0 * RADIUS / math.log(2.0)
SQUARED_E = math.exp(2.0)
PULL = 2.0 / RADIUS
PUSH = 1.0 / RADIUS
FORCE = -2.0 * SQUARED_E * SQUARED_E
PAIR = 0.5 * 0.5 * SQUARED_E * SQUARED_E


def minus(o):
    return tuple(-a for a in o)


def up(rows):
    return -(-rows // 8) * 8


def low(a):
    return 0 if a == -1 else 1


def moved(value, amount, axis=1):
    amount %= value.shape[axis]
    return value if amount == 0 else pltpu.roll(value, amount, axis)


def density_sum(near, here, size):
    base = [[h - s * UNIT for s in (-1.0, 0.0, 1.0)] for h in here]
    total = jnp.zeros((size, LANES), jnp.float32)
    for dx, dy in PLANE:
        for dz in (-1, 0, 1):
            if (dx, dy, dz) == (0, 0, 0):
                continue
            sx = near(dx, dy, dz, 0) - base[0][dx + 1]
            sy = near(dx, dy, dz, 1) - base[1][dy + 1]
            sz = near(dx, dy, dz, 2) - base[2][dz + 1]
            square = sx * sx + sy * sy + sz * sz
            distance = square * lax.rsqrt(square)
            inside = 1.0 - square
            total = total + near(dx, dy, dz, 3) * (
                jnp.exp2(distance * RATE) * (inside * inside))
    return total


def force_sum(near, slope_near, here, slope, size, last):
    base = [[h - s * UNIT for s in (-1.0, 0.0, 1.0)] for h in here]
    force = [jnp.zeros((size, LANES), jnp.float32) for _ in range(3)]
    pair = jnp.zeros((size, LANES), jnp.float32)
    for dx, dy in PLANE:
        for dz in (-1, 0, 1):
            if (dx, dy, dz) == (0, 0, 0):
                continue
            sx = near(dx, dy, dz, 0) - base[0][dx + 1]
            sy = near(dx, dy, dz, 1) - base[1][dy + 1]
            sz = near(dx, dy, dz, 2) - base[2][dz + 1]
            weight = near(dx, dy, dz, 3)
            square = sx * sx + sy * sy + sz * sz
            inverse = lax.rsqrt(square)
            growth = jnp.exp2(square * inverse * RATE)
            inside = 1.0 - square
            steep = PULL + inside * inverse
            both = slope + slope_near(dx, dy, dz)
            cut = growth * inside
            scale = (both * steep + growth * (steep - PUSH)) * cut * weight
            force = [force[0] + scale * sx, force[1] + scale * sy, force[2] + scale * sz]
            if last:
                pair = pair + weight * (cut * cut)
    return force, pair


def kernel(sizes, counts, disp_hbm, occ_hbm, str_hbm, force_ref, energy_ref,
           disp_ref, occ_ref, str_ref, xs, ys, xl, yl, near, slopes, scaled,
           stage, ps, px, pz, sp, sn, ss, sscaled, sroot, xp, xq, final,
           main_send, main_recv, panel_send, panel_recv, strip_send, strip_recv, load_sem, ready):
    cx, cy, cz = sizes
    pitch = cy + 4
    wide = cy + 2 * DEEP
    group = cx * wide
    f32 = jnp.float32

    loads = [pltpu.make_async_copy(disp_hbm, disp_ref, load_sem.at[0]),
             pltpu.make_async_copy(occ_hbm, occ_ref, load_sem.at[1]),
             pltpu.make_async_copy(str_hbm, str_ref, load_sem.at[2])]
    for load in loads:
        load.start()

    me = [lax.axis_index(axis) for axis in AXES]
    there = [[None if s == 0 else (m + s >= 0) & (m + s < n) for s in (-1, 0, 1)]
             for m, n in zip(me, counts)]

    def exists(o):
        tests = [there[a][o[a] + 1] for a in range(3) if o[a] != 0]
        return functools.reduce(lambda p, q: p & q, tests)

    def target(o):
        return {AXES[a]: me[a] + o[a] for a in range(3)}

    ends_z = [(0, 0, -1), (0, 0, 1)]
    barrier = pltpu.get_barrier_semaphore()
    for o in ends_z + FLAT:
        @pl.when(exists(o))
        def _(o=o):
            pl.semaphore_signal(barrier, inc=1, device_id=target(o), device_id_type=MESH)
    spans = [1 + (m > 0).astype(jnp.int32) + (m < n - 1).astype(jnp.int32)
             for m, n in zip(me, counts)]

    for s in (-1, 1):
        @pl.when(jnp.logical_not(there[0][s + 1]))
        def _(s=s):
            xl[:, low(s)] = jnp.zeros(xl.shape[:1] + xl.shape[2:], f32)
            yl[:, s + 1] = jnp.zeros(yl.shape[:1] + yl.shape[2:], f32)
            xq[:, low(s)] = jnp.zeros(xq.shape[:1] + xq.shape[2:], f32)
            px[3 * (s + 1):3 * (s + 1) + 3] = jnp.zeros((3,) + px.shape[1:], f32)
            pz[3 * (s + 1):3 * (s + 1) + 3] = jnp.zeros((3,) + pz.shape[1:], f32)

        @pl.when(jnp.logical_not(there[1][s + 1]))
        def _(s=s):
            yl[:, :, low(s)] = jnp.zeros(yl.shape[:2] + yl.shape[3:], f32)
            for dx in range(3):
                px[3 * dx + s + 1] = jnp.zeros(px.shape[1:], f32)
                pz[3 * dx + s + 1] = jnp.zeros(pz.shape[1:], f32)

        @pl.when(jnp.logical_not(there[2][s + 1]))
        def _(s=s):
            pz[:, low(s)] = jnp.zeros(pz.shape[:1] + pz.shape[2:], f32)

    stage[...] = jnp.zeros(stage.shape, f32)
    near[...] = jnp.zeros(near.shape, f32)
    sn[...] = jnp.zeros(sn.shape, f32)
    ss[...] = jnp.zeros(ss.shape, f32)

    def main_rows(t, face):
        return (4 if t == 0 else 3) * cx * cy if face else up((4 if t == 0 else 3) * cx * 2)

    def main_send_to(t, o):
        back = minus(o)
        rows = pl.ds(0, main_rows(t, o[1] == 0))
        if o[1] == 0:
            src, dst = xs.at[t, rows], xl.at[t, low(back[0]), rows]
        else:
            src, dst = ys.at[t, low(back[1]), rows], yl.at[t, back[0] + 1, low(back[1]), rows]
        return pltpu.make_async_remote_copy(
            src_ref=src, dst_ref=dst, send_sem=main_send.at[t, FLAT.index(o)],
            recv_sem=main_recv.at[t, FLAT.index(back)], device_id=target(o), device_id_type=MESH)

    def main_from(t, o):
        rows = pl.ds(0, main_rows(t, o[1] == 0))
        spot = xl.at[t, low(o[0]), rows] if o[1] == 0 else yl.at[t, o[0] + 1, low(o[1]), rows]
        return pltpu.make_async_remote_copy(
            src_ref=spot, dst_ref=spot, send_sem=main_send.at[t, FLAT.index(o)],
            recv_sem=main_recv.at[t, FLAT.index(o)], device_id=target(o), device_id_type=MESH)

    def panel_spot(o):
        j = PLANE.index(o[:2])
        return px.at[j] if o[2] == 0 else pz.at[j, low(o[2])]

    def panel_to(o):
        back = minus(o)
        rows = pl.ds(0, 32) if o[2] == 0 else pl.ds(8 if o[2] == -1 else 16, 16)
        return pltpu.make_async_remote_copy(
            src_ref=ps.at[back[1] + 1, rows], dst_ref=panel_spot(back),
            send_sem=panel_send.at[PANELS.index(o)], recv_sem=panel_recv.at[PANELS.index(back)],
            device_id=target(o), device_id_type=MESH)

    def panel_from(o):
        return pltpu.make_async_remote_copy(
            src_ref=panel_spot(o), dst_ref=panel_spot(o),
            send_sem=panel_send.at[PANELS.index(o)], recv_sem=panel_recv.at[PANELS.index(o)],
            device_id=target(o), device_id_type=MESH)

    def strip_to(t, o):
        back = minus(o)
        return pltpu.make_async_remote_copy(
            src_ref=xp.at[t], dst_ref=xq.at[t, low(back[0])],
            send_sem=strip_send.at[t, low(o[0])], recv_sem=strip_recv.at[t, low(back[0])],
            device_id=target(o), device_id_type=MESH)

    def strip_from(t, o):
        spot = xq.at[t, low(o[0])]
        return pltpu.make_async_remote_copy(
            src_ref=spot, dst_ref=spot,
            send_sem=strip_send.at[t, low(o[0])], recv_sem=strip_recv.at[t, low(o[0])],
            device_id=target(o), device_id_type=MESH)

    def each(offsets, act):
        for o in offsets:
            @pl.when(exists(o))
            def _(o=o):
                act(o)

    SIDES = [(-1, 0, 0), (1, 0, 0)]

    for load in loads:
        load.wait()
    mine = [[disp_ref[q, x] * UNIT for x in range(cx)] for q in range(3)]
    mine.append([occ_ref[x].astype(f32) * str_ref[x] for x in range(cx)])

    def fill_sends(t):
        for q in range(4 if t == 0 else 3):
            for x in range(cx):
                i = q * cx + x
                xs[t, i * cy:(i + 1) * cy] = mine[q][x]
                ys[t, 0, i * 2:i * 2 + 2] = mine[q][x][cy - 2:cy]
                ys[t, 1, i * 2:i * 2 + 2] = mine[q][x][0:2]

    def put(q, row, piece):
        rows = piece.shape[0]
        near[0, q, row:row + rows] = moved(piece, 1)
        near[1, q, row:row + rows] = piece
        near[2, q, row:row + rows] = moved(piece, -1)

    def put_mine(t):
        for q in range(4 if t == 0 else 3):
            for x in range(cx):
                put(q, (cx + x) * pitch + 2, mine[q][x])

    def put_others(t):
        for q in range(4 if t == 0 else 3):
            for x in range(cx):
                i = q * cx + x
                for dx in (-1, 0, 1):
                    row = (cx * (dx + 1) + x) * pitch
                    if dx != 0:
                        put(q, row + 2, xl[t, low(dx), i * cy:(i + 1) * cy])
                    put(q, row, yl[t, dx + 1, 0, i * 2:i * 2 + 2])
                    put(q, row + 2 + cy, yl[t, dx + 1, 1, i * 2:i * 2 + 2])

    fill_sends(0)
    pl.semaphore_wait(barrier, spans[0] * spans[1] + spans[2] - 2)
    each(FLAT, lambda o: main_send_to(0, o).start())
    each(ends_z, lambda o: pl.semaphore_signal(
        ready, inc=1, device_id=target(o), device_id_type=MESH))

    lane = lax.broadcasted_iota(jnp.int32, (8, LANES), 1)
    half = lax.broadcasted_iota(jnp.int32, (8, LANES), 0) < 4
    column = lax.rem(lane, wide)
    for x in range(cx):
        for q in range(3):
            row = q * group + x * wide + DEEP
            stage[0, row:row + cy] = mine[q][x]
            stage[1, row:row + cy] = mine[3][x]
    turned = jnp.transpose(stage[0])
    heavy = jnp.transpose(stage[1])

    def ends_of(value):
        return (value[0:8], jnp.where(half, value[8:16], value[cz - 16:cz - 8]), value[cz - 8:cz])

    first, middle, end = ends_of(turned)
    load_first, load_middle, load_end = ends_of(heavy)
    load = jnp.where(lane < group, load_first, jnp.where(lane < 2 * group, load_middle, load_end))
    for i, piece in enumerate((middle, first, load, end)):
        ps[1, 8 * i:8 * i + 8] = piece
        ps[0, 8 * i:8 * i + 8] = jnp.where(column < DEEP, moved(piece, -cy), 0.0)
        ps[2, 8 * i:8 * i + 8] = jnp.where(column >= DEEP + cy, moved(piece, cy), 0.0)
    each(FLAT, lambda o: panel_to(o).start())
    pl.semaphore_wait(ready, spans[2] - 1)
    each(TALL, lambda o: panel_to(o).start())

    put_mine(0)

    begin = pitch + 1
    chunk = 16
    extent = up((cx + 2) * pitch + cy + 3 - begin)

    def main_step(t):
        last = t == ITERS - 1
        each(FLAT, lambda o: main_from(t, o).wait_recv())
        put_others(t)
        if t == 0:
            weight = near[1, 3, begin:begin + extent]
            scaled[begin:begin + extent] = jnp.where(
                weight > 0.0, (-0.5 / SQUARED_E) / jnp.where(weight > 0.0, weight, 1.0), 0.0)
        for start in range(begin, begin + extent, chunk):
            size = min(chunk, begin + extent - start)

            def around(dx, dy, dz, q, start=start, size=size):
                row = start + dx * pitch + dy
                return near[dz + 1, q, row:row + size]

            total = 1.0 + SQUARED_E * density_sum(
                around, [near[1, q, start:start + size] for q in range(3)], size)
            root = lax.rsqrt(total)
            slope = scaled[start:start + size] * root
            slopes[0, start:start + size] = moved(slope, 1)
            slopes[1, start:start + size] = slope
            slopes[2, start:start + size] = moved(slope, -1)
            if last:
                slopes[3, start:start + size] = total * root
        for x in range(cx):
            start = (cx + x) * pitch + 2

            def around(dx, dy, dz, q, start=start):
                row = start + dx * pitch + dy
                return near[dz + 1, q, row:row + cy]

            def slope_around(dx, dy, dz, start=start):
                row = start + dx * pitch + dy
                return slopes[dz + 1, row:row + cy]

            here = [mine[q][x] for q in range(3)]
            force, pair = force_sum(around, slope_around, here, slopes[1, start:start + cy], cy, last)
            weight = mine[3][x]
            if last:
                for q in range(3):
                    force_ref[q, x] = (weight * FORCE) * force[q]
                energy_ref[x] = (weight * PAIR) * pair - jnp.where(
                    weight > 0.0, slopes[3, start:start + cy], 0.0)
            else:
                for q in range(3):
                    mine[q][x] = here[q] + (weight * (FORCE * STEP * UNIT)) * force[q]
        if not last:
            fill_sends(t + 1)
            each(FLAT, lambda o: main_send_to(t + 1, o).start())
            put_mine(t + 1)

    def spread(parts, at):
        found = [moved(parts[i], group * (i - at)) for i in range(3)]
        return jnp.where(lane < group, found[0], jnp.where(
            lane < 2 * group, found[1], jnp.where(lane < 3 * group, found[2], 0.0)))

    def put_strip(q, row, value):
        for j, (dx, dy) in enumerate(PLANE):
            sp[j, q, row:row + 8] = moved(value, -(dx * wide + dy))

    def strip_step(t):
        last = t == ITERS - 1
        if t == 0:
            each(PANELS, lambda o: panel_from(o).wait_recv())

            def flat(rows):
                return [sum(ps[1, rows:rows + 8] if (dx, dy) == (0, 0)
                            else px[PLANE.index((dx, dy)), rows:rows + 8] for dy in (-1, 0, 1))
                        for dx in (-1, 0, 1)]

            def tall(side, rows):
                return [sum(pz[PLANE.index((dx, dy)), side, rows:rows + 8] for dy in (-1, 0, 1))
                        for dx in (-1, 0, 1)]

            blocks = [tall(0, 8), flat(8), flat(0), flat(24), tall(1, 0)]
            for b, parts in enumerate(blocks):
                for q in range(3):
                    put_strip(q, 8 * b, spread(parts, q))
            loads_at = flat(16)
            for b, (parts, at) in enumerate(((tall(0, 0), 2), (loads_at, 0), (loads_at, 1),
                                             (loads_at, 2), (tall(1, 8), 0))):
                weight = spread(parts, at)
                put_strip(3, 8 * b, weight)
                sscaled[8 * b:8 * b + 8] = jnp.where(
                    weight > 0.0, (-0.5 / SQUARED_E) / jnp.where(weight > 0.0, weight, 1.0), 0.0)
        else:
            each(SIDES, lambda o: strip_from(t - 1, o).wait_recv())
            for b in range(4):
                for q in range(3):
                    under = moved(xq[t - 1, 0, 8 * b:8 * b + 8], -group * q)
                    over = moved(xq[t - 1, 1, 8 * b:8 * b + 8], group * (2 - q))
                    put_strip(q, 4 + 8 * b, jnp.where(lane < group, under, jnp.where(
                        lane < 2 * group, sn[q, 4 + 8 * b:12 + 8 * b],
                        jnp.where(lane < 3 * group, over, 0.0))))

        reach = 2 * (ITERS - 1 - t)
        starts = []
        for base in (8, 32 - DEEP):
            starts += sorted({base - reach - 1, base + DEEP + reach + 1 - 8})
        for row in starts:
            def around(dx, dy, dz, q, row=row):
                return sp[PLANE.index((dx, dy)), q, row + dz:row + dz + 8]

            total = 1.0 + SQUARED_E * density_sum(
                around, [sp[4, q, row:row + 8] for q in range(3)], 8)
            root = lax.rsqrt(total)
            slope = sscaled[row:row + 8] * root
            for j, (dx, dy) in enumerate(PLANE):
                ss[j, row:row + 8] = moved(slope, -(dx * wide + dy))
            if last:
                sroot[row:row + 8] = total * root
        starts = [8, 24]
        if not last:
            starts = []
            for base in (8, 32 - DEEP):
                starts += sorted({base - reach, base + DEEP + reach - 8})
        results = []
        for row in starts:
            def around(dx, dy, dz, q, row=row):
                return sp[PLANE.index((dx, dy)), q, row + dz:row + dz + 8]

            def slope_around(dx, dy, dz, row=row):
                return ss[PLANE.index((dx, dy)), row + dz:row + dz + 8]

            here = [sp[4, q, row:row + 8] for q in range(3)]
            force, pair = force_sum(around, slope_around, here, ss[4, row:row + 8], 8, last)
            weight = sp[4, 3, row:row + 8]
            if last:
                energy = (weight * PAIR) * pair - jnp.where(
                    weight > 0.0, sroot[row:row + 8], 0.0)
                results.append([(weight * FORCE) * f for f in force] + [energy])
            else:
                for q in range(3):
                    sn[q, row:row + 8] = here[q] + (weight * (FORCE * STEP * UNIT)) * force[q]
        if not last:
            for b in range(4):
                new = [moved(sn[q, 4 + 8 * b:12 + 8 * b], group * (q - 1)) for q in range(3)]
                xp[t, 8 * b:8 * b + 8] = jnp.where(
                    lane < group, new[0], jnp.where(lane < 2 * group, new[1], new[2]))
            each(SIDES, lambda o: strip_to(t, o).start())
            return
        rows = []
        for q in range(4):
            rows += [results[1][q], results[0][q]]
        rows.append(jnp.zeros((LANES - 64, LANES), f32))
        final[...] = jnp.transpose(jnp.concatenate(rows, axis=0))
        outer = (lane < DEEP) | (lane >= cz - DEEP)
        for q in range(4):
            for x in range(cx):
                start = group + x * wide + DEEP
                piece = moved(final[start:start + cy], cz - 8 - 16 * q)
                spot = force_ref.at[q, x] if q < 3 else energy_ref.at[x]
                spot[...] = jnp.where(outer, piece, spot[...])

    for t in range(ITERS):
        main_step(t)
        strip_step(t)
        if t == 0:
            each(PANELS, lambda o: panel_to(o).wait_send())
            each(FLAT, lambda o: main_send_to(0, o).wait_send())
        else:
            each(FLAT, lambda o: main_send_to(t, o).wait_send())
            each(SIDES, lambda o: strip_to(t - 1, o).wait_send())


def solution(mesh):
    counts = tuple(mesh.shape[axis] for axis in AXES)

    def body(displace, occupied, strength):
        sizes = occupied.shape
        cx, cy, cz = sizes
        assert cx == 2 and cy == 8 and cz == LANES
        pitch = cy + 4
        rows = up(2 * (pitch + 1) + up((cx + 2) * pitch + cy + 3 - (pitch + 1)))
        f32 = jnp.float32
        vmem = pl.BlockSpec(memory_space=pltpu.VMEM)
        return pl.pallas_call(
            functools.partial(kernel, sizes, counts),
            out_shape=(pltpu.VMEM((3,) + sizes, f32), pltpu.VMEM(sizes, f32)),
            in_specs=[pl.BlockSpec(memory_space=pl.ANY)] * 3,
            out_specs=(vmem, vmem),
            scratch_shapes=[
                pltpu.VMEM((3,) + sizes, f32),
                pltpu.VMEM(sizes, jnp.int32),
                pltpu.VMEM(sizes, f32),
                pltpu.VMEM((ITERS, 4 * cx * cy, LANES), f32),
                pltpu.VMEM((ITERS, 2, up(8 * cx), LANES), f32),
                pltpu.VMEM((ITERS, 2, 4 * cx * cy, LANES), f32),
                pltpu.VMEM((ITERS, 3, 2, up(8 * cx), LANES), f32),
                pltpu.VMEM((3, 4, rows, LANES), f32),
                pltpu.VMEM((4, rows, LANES), f32),
                pltpu.VMEM((rows, LANES), f32),
                pltpu.VMEM((2, LANES, LANES), f32),
                pltpu.VMEM((3, 32, LANES), f32),
                pltpu.VMEM((9, 32, LANES), f32),
                pltpu.VMEM((9, 2, 16, LANES), f32),
                pltpu.VMEM((9, 4, 40, LANES), f32),
                pltpu.VMEM((3, 40, LANES), f32),
                pltpu.VMEM((9, 40, LANES), f32),
                pltpu.VMEM((40, LANES), f32),
                pltpu.VMEM((40, LANES), f32),
                pltpu.VMEM((ITERS - 1, 32, LANES), f32),
                pltpu.VMEM((ITERS - 1, 2, 32, LANES), f32),
                pltpu.VMEM((LANES, LANES), f32),
                pltpu.SemaphoreType.DMA((ITERS, len(FLAT))),
                pltpu.SemaphoreType.DMA((ITERS, len(FLAT))),
                pltpu.SemaphoreType.DMA((len(PANELS),)),
                pltpu.SemaphoreType.DMA((len(PANELS),)),
                pltpu.SemaphoreType.DMA((ITERS - 1, 2)),
                pltpu.SemaphoreType.DMA((ITERS - 1, 2)),
                pltpu.SemaphoreType.DMA((3,)),
                pltpu.SemaphoreType.REGULAR,
            ],
            compiler_params=pltpu.CompilerParams(collective_id=0, has_side_effects=True),
        )(displace, occupied, strength)

    in_specs = (P(None, "gx", "gy", "gz"), P("gx", "gy", "gz"), P("gx", "gy", "gz"))
    out_specs = (P(None, "gx", "gy", "gz"), P("gx", "gy", "gz"))
    return jax.shard_map(body, mesh=mesh, in_specs=in_specs, out_specs=out_specs, check_vma=False)
```

```python
import functools
import math

import jax
import jax.numpy as jnp
from jax import lax
from jax.experimental import pallas as pl
from jax.experimental.pallas import tpu as pltpu
from jax.sharding import PartitionSpec as P

ITERS = 3
RADIUS_SQ = 4.84
STEP = 0.02
AXES = ("gx", "gy", "gz")
MESH = pl.DeviceIdType.MESH
LANES = 128
DEEP = 2 * ITERS
PLANE = [(dx, dy) for dx in (-1, 0, 1) for dy in (-1, 0, 1)]
FLAT = sorted(((dx, dy, 0) for dx, dy in PLANE if (dx, dy) != (0, 0)),
              key=lambda o: (-sum(abs(a) for a in o), o))
TALL = sorted(((dx, dy, dz) for dx, dy in PLANE for dz in (-1, 1)),
              key=lambda o: (-sum(abs(a) for a in o), o))
PANELS = TALL + FLAT

RADIUS = math.sqrt(RADIUS_SQ)
UNIT = 1.0 / RADIUS
RATE = -2.0 * RADIUS / math.log(2.0)
SQUARED_E = math.exp(2.0)
PULL = 2.0 / RADIUS
PUSH = 1.0 / RADIUS
FORCE = -2.0 * SQUARED_E * SQUARED_E
PAIR = 0.5 * 0.5 * SQUARED_E * SQUARED_E


def minus(o):
    return tuple(-a for a in o)


def up(rows):
    return -(-rows // 8) * 8


def low(a):
    return 0 if a == -1 else 1


def moved(value, amount, axis=1):
    amount %= value.shape[axis]
    return value if amount == 0 else pltpu.roll(value, amount, axis)


def density_sum(near, here, size):
    base = [[h - s * UNIT for s in (-1.0, 0.0, 1.0)] for h in here]
    total = jnp.zeros((size, LANES), jnp.float32)
    for dx, dy in PLANE:
        for dz in (-1, 0, 1):
            if (dx, dy, dz) == (0, 0, 0):
                continue
            sx = near(dx, dy, dz, 0) - base[0][dx + 1]
            sy = near(dx, dy, dz, 1) - base[1][dy + 1]
            sz = near(dx, dy, dz, 2) - base[2][dz + 1]
            square = sx * sx + sy * sy + sz * sz
            distance = square * lax.rsqrt(square)
            inside = 1.0 - square
            total = total + near(dx, dy, dz, 3) * (
                jnp.exp2(distance * RATE) * (inside * inside))
    return total


def force_sum(near, slope_near, here, slope, size, last):
    base = [[h - s * UNIT for s in (-1.0, 0.0, 1.0)] for h in here]
    force = [jnp.zeros((size, LANES), jnp.float32) for _ in range(3)]
    pair = jnp.zeros((size, LANES), jnp.float32)
    for dx, dy in PLANE:
        for dz in (-1, 0, 1):
            if (dx, dy, dz) == (0, 0, 0):
                continue
            sx = near(dx, dy, dz, 0) - base[0][dx + 1]
            sy = near(dx, dy, dz, 1) - base[1][dy + 1]
            sz = near(dx, dy, dz, 2) - base[2][dz + 1]
            weight = near(dx, dy, dz, 3)
            square = sx * sx + sy * sy + sz * sz
            inverse = lax.rsqrt(square)
            growth = jnp.exp2(square * inverse * RATE)
            inside = 1.0 - square
            steep = PULL + inside * inverse
            both = slope + slope_near(dx, dy, dz)
            cut = growth * inside
            scale = (both * steep + growth * (steep - PUSH)) * cut * weight
            force = [force[0] + scale * sx, force[1] + scale * sy, force[2] + scale * sz]
            if last:
                pair = pair + weight * (cut * cut)
    return force, pair


def kernel(sizes, counts, disp_hbm, occ_hbm, str_hbm, force_ref, energy_ref,
           disp_ref, occ_ref, str_ref, xs, ys, xl, yl, near, slopes, scaled,
           stage, ps, px, pz, sp, sn, ss, sscaled, sroot, xp, xq, final,
           main_send, main_recv, panel_send, panel_recv, strip_send, strip_recv, load_sem):
    cx, cy, cz = sizes
    pitch = cy + 4
    wide = cy + 2 * DEEP
    group = cx * wide
    f32 = jnp.float32

    loads = [pltpu.make_async_copy(disp_hbm, disp_ref, load_sem.at[0]),
             pltpu.make_async_copy(occ_hbm, occ_ref, load_sem.at[1]),
             pltpu.make_async_copy(str_hbm, str_ref, load_sem.at[2])]
    for load in loads:
        load.start()

    me = [lax.axis_index(axis) for axis in AXES]
    there = [[None if s == 0 else (m + s >= 0) & (m + s < n) for s in (-1, 0, 1)]
             for m, n in zip(me, counts)]

    def exists(o):
        tests = [there[a][o[a] + 1] for a in range(3) if o[a] != 0]
        return functools.reduce(lambda p, q: p & q, tests)

    def target(o):
        return {AXES[a]: me[a] + o[a] for a in range(3)}

    barrier = pltpu.get_barrier_semaphore()
    for o in PANELS:
        @pl.when(exists(o))
        def _(o=o):
            pl.semaphore_signal(barrier, inc=1, device_id=target(o), device_id_type=MESH)
    spans = [1 + (m > 0).astype(jnp.int32) + (m < n - 1).astype(jnp.int32)
             for m, n in zip(me, counts)]

    for s in (-1, 1):
        @pl.when(jnp.logical_not(there[0][s + 1]))
        def _(s=s):
            xl[:, low(s)] = jnp.zeros(xl.shape[:1] + xl.shape[2:], f32)
            yl[:, s + 1] = jnp.zeros(yl.shape[:1] + yl.shape[2:], f32)
            xq[:, low(s)] = jnp.zeros(xq.shape[:1] + xq.shape[2:], f32)
            px[3 * (s + 1):3 * (s + 1) + 3] = jnp.zeros((3,) + px.shape[1:], f32)
            pz[3 * (s + 1):3 * (s + 1) + 3] = jnp.zeros((3,) + pz.shape[1:], f32)

        @pl.when(jnp.logical_not(there[1][s + 1]))
        def _(s=s):
            yl[:, :, low(s)] = jnp.zeros(yl.shape[:2] + yl.shape[3:], f32)
            for dx in range(3):
                px[3 * dx + s + 1] = jnp.zeros(px.shape[1:], f32)
                pz[3 * dx + s + 1] = jnp.zeros(pz.shape[1:], f32)

        @pl.when(jnp.logical_not(there[2][s + 1]))
        def _(s=s):
            pz[:, low(s)] = jnp.zeros(pz.shape[:1] + pz.shape[2:], f32)

    stage[...] = jnp.zeros(stage.shape, f32)
    near[...] = jnp.zeros(near.shape, f32)
    sn[...] = jnp.zeros(sn.shape, f32)
    ss[...] = jnp.zeros(ss.shape, f32)

    def main_rows(t, face):
        return (4 if t == 0 else 3) * cx * cy if face else up((4 if t == 0 else 3) * cx * 2)

    def main_send_to(t, o):
        back = minus(o)
        rows = pl.ds(0, main_rows(t, o[1] == 0))
        if o[1] == 0:
            src, dst = xs.at[t, rows], xl.at[t, low(back[0]), rows]
        else:
            src, dst = ys.at[t, low(back[1]), rows], yl.at[t, back[0] + 1, low(back[1]), rows]
        return pltpu.make_async_remote_copy(
            src_ref=src, dst_ref=dst, send_sem=main_send.at[t, FLAT.index(o)],
            recv_sem=main_recv.at[t, FLAT.index(back)], device_id=target(o), device_id_type=MESH)

    def main_from(t, o):
        rows = pl.ds(0, main_rows(t, o[1] == 0))
        spot = xl.at[t, low(o[0]), rows] if o[1] == 0 else yl.at[t, o[0] + 1, low(o[1]), rows]
        return pltpu.make_async_remote_copy(
            src_ref=spot, dst_ref=spot, send_sem=main_send.at[t, FLAT.index(o)],
            recv_sem=main_recv.at[t, FLAT.index(o)], device_id=target(o), device_id_type=MESH)

    def panel_spot(o):
        j = PLANE.index(o[:2])
        return px.at[j] if o[2] == 0 else pz.at[j, low(o[2])]

    def panel_to(o):
        back = minus(o)
        rows = pl.ds(0, 32) if o[2] == 0 else pl.ds(8 if o[2] == -1 else 16, 16)
        return pltpu.make_async_remote_copy(
            src_ref=ps.at[back[1] + 1, rows], dst_ref=panel_spot(back),
            send_sem=panel_send.at[PANELS.index(o)], recv_sem=panel_recv.at[PANELS.index(back)],
            device_id=target(o), device_id_type=MESH)

    def panel_from(o):
        return pltpu.make_async_remote_copy(
            src_ref=panel_spot(o), dst_ref=panel_spot(o),
            send_sem=panel_send.at[PANELS.index(o)], recv_sem=panel_recv.at[PANELS.index(o)],
            device_id=target(o), device_id_type=MESH)

    def strip_to(t, o):
        back = minus(o)
        return pltpu.make_async_remote_copy(
            src_ref=xp.at[t], dst_ref=xq.at[t, low(back[0])],
            send_sem=strip_send.at[t, low(o[0])], recv_sem=strip_recv.at[t, low(back[0])],
            device_id=target(o), device_id_type=MESH)

    def strip_from(t, o):
        spot = xq.at[t, low(o[0])]
        return pltpu.make_async_remote_copy(
            src_ref=spot, dst_ref=spot,
            send_sem=strip_send.at[t, low(o[0])], recv_sem=strip_recv.at[t, low(o[0])],
            device_id=target(o), device_id_type=MESH)

    def each(offsets, act):
        for o in offsets:
            @pl.when(exists(o))
            def _(o=o):
                act(o)

    SIDES = [(-1, 0, 0), (1, 0, 0)]

    for load in loads:
        load.wait()
    mine = [[disp_ref[q, x] * UNIT for x in range(cx)] for q in range(3)]
    mine.append([occ_ref[x].astype(f32) * str_ref[x] for x in range(cx)])

    def fill_sends(t):
        for q in range(4 if t == 0 else 3):
            for x in range(cx):
                i = q * cx + x
                xs[t, i * cy:(i + 1) * cy] = mine[q][x]
                ys[t, 0, i * 2:i * 2 + 2] = mine[q][x][cy - 2:cy]
                ys[t, 1, i * 2:i * 2 + 2] = mine[q][x][0:2]

    def put(q, row, piece):
        rows = piece.shape[0]
        near[0, q, row:row + rows] = moved(piece, 1)
        near[1, q, row:row + rows] = piece
        near[2, q, row:row + rows] = moved(piece, -1)

    def put_mine(t):
        for q in range(4 if t == 0 else 3):
            for x in range(cx):
                put(q, (cx + x) * pitch + 2, mine[q][x])

    def put_others(t):
        for q in range(4 if t == 0 else 3):
            for x in range(cx):
                i = q * cx + x
                for dx in (-1, 0, 1):
                    row = (cx * (dx + 1) + x) * pitch
                    if dx != 0:
                        put(q, row + 2, xl[t, low(dx), i * cy:(i + 1) * cy])
                    put(q, row, yl[t, dx + 1, 0, i * 2:i * 2 + 2])
                    put(q, row + 2 + cy, yl[t, dx + 1, 1, i * 2:i * 2 + 2])

    fill_sends(0)

    lane = lax.broadcasted_iota(jnp.int32, (8, LANES), 1)
    half = lax.broadcasted_iota(jnp.int32, (8, LANES), 0) < 4
    column = lax.rem(lane, wide)
    for x in range(cx):
        for q in range(3):
            row = q * group + x * wide + DEEP
            stage[0, row:row + cy] = mine[q][x]
            stage[1, row:row + cy] = mine[3][x]
    turned = jnp.transpose(stage[0])
    heavy = jnp.transpose(stage[1])

    def ends_of(value):
        return (value[0:8], jnp.where(half, value[8:16], value[cz - 16:cz - 8]), value[cz - 8:cz])

    first, middle, end = ends_of(turned)
    load_first, load_middle, load_end = ends_of(heavy)
    load = jnp.where(lane < group, load_first, jnp.where(lane < 2 * group, load_middle, load_end))
    for i, piece in enumerate((middle, first, load, end)):
        ps[1, 8 * i:8 * i + 8] = piece
        ps[0, 8 * i:8 * i + 8] = jnp.where(column < DEEP, moved(piece, -cy), 0.0)
        ps[2, 8 * i:8 * i + 8] = jnp.where(column >= DEEP + cy, moved(piece, cy), 0.0)
    put_mine(0)
    pl.semaphore_wait(barrier, spans[0] * spans[1] * spans[2] - 1)
    each(FLAT, lambda o: main_send_to(0, o).start())
    each(PANELS, lambda o: panel_to(o).start())

    begin = pitch + 1
    chunk = 16
    extent = up((cx + 2) * pitch + cy + 3 - begin)

    def main_step(t):
        last = t == ITERS - 1
        each(FLAT, lambda o: main_from(t, o).wait_recv())
        put_others(t)
        if t == 0:
            weight = near[1, 3, begin:begin + extent]
            scaled[begin:begin + extent] = jnp.where(
                weight > 0.0, (-0.5 / SQUARED_E) / jnp.where(weight > 0.0, weight, 1.0), 0.0)
        for start in range(begin, begin + extent, chunk):
            size = min(chunk, begin + extent - start)

            def around(dx, dy, dz, q, start=start, size=size):
                row = start + dx * pitch + dy
                return near[dz + 1, q, row:row + size]

            total = 1.0 + SQUARED_E * density_sum(
                around, [near[1, q, start:start + size] for q in range(3)], size)
            root = lax.rsqrt(total)
            slope = scaled[start:start + size] * root
            slopes[0, start:start + size] = moved(slope, 1)
            slopes[1, start:start + size] = slope
            slopes[2, start:start + size] = moved(slope, -1)
            if last:
                slopes[3, start:start + size] = total * root
        for x in range(cx):
            start = (cx + x) * pitch + 2

            def around(dx, dy, dz, q, start=start):
                row = start + dx * pitch + dy
                return near[dz + 1, q, row:row + cy]

            def slope_around(dx, dy, dz, start=start):
                row = start + dx * pitch + dy
                return slopes[dz + 1, row:row + cy]

            here = [mine[q][x] for q in range(3)]
            force, pair = force_sum(around, slope_around, here, slopes[1, start:start + cy], cy, last)
            weight = mine[3][x]
            if last:
                for q in range(3):
                    force_ref[q, x] = (weight * FORCE) * force[q]
                energy_ref[x] = (weight * PAIR) * pair - jnp.where(
                    weight > 0.0, slopes[3, start:start + cy], 0.0)
            else:
                for q in range(3):
                    mine[q][x] = here[q] + (weight * (FORCE * STEP * UNIT)) * force[q]
        if not last:
            fill_sends(t + 1)
            each(FLAT, lambda o: main_send_to(t + 1, o).start())
            put_mine(t + 1)

    def spread(parts, at):
        found = [moved(parts[i], group * (i - at)) for i in range(3)]
        return jnp.where(lane < group, found[0], jnp.where(
            lane < 2 * group, found[1], jnp.where(lane < 3 * group, found[2], 0.0)))

    def put_strip(q, row, value):
        for j, (dx, dy) in enumerate(PLANE):
            sp[j, q, row:row + 8] = moved(value, -(dx * wide + dy))

    def strip_step(t):
        last = t == ITERS - 1
        if t == 0:
            each(PANELS, lambda o: panel_from(o).wait_recv())

            def flat(rows):
                return [sum(ps[1, rows:rows + 8] if (dx, dy) == (0, 0)
                            else px[PLANE.index((dx, dy)), rows:rows + 8] for dy in (-1, 0, 1))
                        for dx in (-1, 0, 1)]

            def tall(side, rows):
                return [sum(pz[PLANE.index((dx, dy)), side, rows:rows + 8] for dy in (-1, 0, 1))
                        for dx in (-1, 0, 1)]

            blocks = [tall(0, 8), flat(8), flat(0), flat(24), tall(1, 0)]
            for b, parts in enumerate(blocks):
                for q in range(3):
                    put_strip(q, 8 * b, spread(parts, q))
            loads_at = flat(16)
            for b, (parts, at) in enumerate(((tall(0, 0), 2), (loads_at, 0), (loads_at, 1),
                                             (loads_at, 2), (tall(1, 8), 0))):
                weight = spread(parts, at)
                put_strip(3, 8 * b, weight)
                sscaled[8 * b:8 * b + 8] = jnp.where(
                    weight > 0.0, (-0.5 / SQUARED_E) / jnp.where(weight > 0.0, weight, 1.0), 0.0)
        else:
            each(SIDES, lambda o: strip_from(t - 1, o).wait_recv())
            for b in range(4):
                for q in range(3):
                    under = moved(xq[t - 1, 0, 8 * b:8 * b + 8], -group * q)
                    over = moved(xq[t - 1, 1, 8 * b:8 * b + 8], group * (2 - q))
                    put_strip(q, 4 + 8 * b, jnp.where(lane < group, under, jnp.where(
                        lane < 2 * group, sn[q, 4 + 8 * b:12 + 8 * b],
                        jnp.where(lane < 3 * group, over, 0.0))))

        reach = 2 * (ITERS - 1 - t)
        starts = []
        for base in (8, 32 - DEEP):
            starts += sorted({base - reach - 1, base + DEEP + reach + 1 - 8})
        for row in starts:
            def around(dx, dy, dz, q, row=row):
                return sp[PLANE.index((dx, dy)), q, row + dz:row + dz + 8]

            total = 1.0 + SQUARED_E * density_sum(
                around, [sp[4, q, row:row + 8] for q in range(3)], 8)
            root = lax.rsqrt(total)
            slope = sscaled[row:row + 8] * root
            for j, (dx, dy) in enumerate(PLANE):
                ss[j, row:row + 8] = moved(slope, -(dx * wide + dy))
            if last:
                sroot[row:row + 8] = total * root
        starts = [8, 24]
        if not last:
            starts = []
            for base in (8, 32 - DEEP):
                starts += sorted({base - reach, base + DEEP + reach - 8})
        results = []
        for row in starts:
            def around(dx, dy, dz, q, row=row):
                return sp[PLANE.index((dx, dy)), q, row + dz:row + dz + 8]

            def slope_around(dx, dy, dz, row=row):
                return ss[PLANE.index((dx, dy)), row + dz:row + dz + 8]

            here = [sp[4, q, row:row + 8] for q in range(3)]
            force, pair = force_sum(around, slope_around, here, ss[4, row:row + 8], 8, last)
            weight = sp[4, 3, row:row + 8]
            if last:
                energy = (weight * PAIR) * pair - jnp.where(
                    weight > 0.0, sroot[row:row + 8], 0.0)
                results.append([(weight * FORCE) * f for f in force] + [energy])
            else:
                for q in range(3):
                    sn[q, row:row + 8] = here[q] + (weight * (FORCE * STEP * UNIT)) * force[q]
        if not last:
            for b in range(4):
                new = [moved(sn[q, 4 + 8 * b:12 + 8 * b], group * (q - 1)) for q in range(3)]
                xp[t, 8 * b:8 * b + 8] = jnp.where(
                    lane < group, new[0], jnp.where(lane < 2 * group, new[1], new[2]))
            each(SIDES, lambda o: strip_to(t, o).start())
            return
        rows = []
        for q in range(4):
            rows += [results[1][q], results[0][q]]
        rows.append(jnp.zeros((LANES - 64, LANES), f32))
        final[...] = jnp.transpose(jnp.concatenate(rows, axis=0))
        outer = (lane < DEEP) | (lane >= cz - DEEP)
        for q in range(4):
            for x in range(cx):
                start = group + x * wide + DEEP
                piece = moved(final[start:start + cy], cz - 8 - 16 * q)
                spot = force_ref.at[q, x] if q < 3 else energy_ref.at[x]
                spot[...] = jnp.where(outer, piece, spot[...])

    for t in range(ITERS):
        main_step(t)
        strip_step(t)
        if t == 0:
            each(PANELS, lambda o: panel_to(o).wait_send())
            each(FLAT, lambda o: main_send_to(0, o).wait_send())
        else:
            each(FLAT, lambda o: main_send_to(t, o).wait_send())
            each(SIDES, lambda o: strip_to(t - 1, o).wait_send())


def put_out(force_ref, energy_ref, force_hbm, energy_hbm, sem):
    copies = [pltpu.make_async_copy(force_ref, force_hbm, sem.at[0]),
              pltpu.make_async_copy(energy_ref, energy_hbm, sem.at[1])]
    for copy in copies:
        copy.start()
    for copy in copies:
        copy.wait()


def solution(mesh):
    counts = tuple(mesh.shape[axis] for axis in AXES)

    def body(displace, occupied, strength):
        sizes = occupied.shape
        cx, cy, cz = sizes
        assert cx == 2 and cy == 8 and cz == LANES
        pitch = cy + 4
        rows = up(2 * (pitch + 1) + up((cx + 2) * pitch + cy + 3 - (pitch + 1)))
        f32 = jnp.float32
        vmem = pl.BlockSpec(memory_space=pltpu.VMEM)
        force, energy = pl.pallas_call(
            functools.partial(kernel, sizes, counts),
            out_shape=(pltpu.VMEM((3,) + sizes, f32), pltpu.VMEM(sizes, f32)),
            in_specs=[pl.BlockSpec(memory_space=pl.ANY)] * 3,
            out_specs=(vmem, vmem),
            scratch_shapes=[
                pltpu.VMEM((3,) + sizes, f32),
                pltpu.VMEM(sizes, jnp.int32),
                pltpu.VMEM(sizes, f32),
                pltpu.VMEM((ITERS, 4 * cx * cy, LANES), f32),
                pltpu.VMEM((ITERS, 2, up(8 * cx), LANES), f32),
                pltpu.VMEM((ITERS, 2, 4 * cx * cy, LANES), f32),
                pltpu.VMEM((ITERS, 3, 2, up(8 * cx), LANES), f32),
                pltpu.VMEM((3, 4, rows, LANES), f32),
                pltpu.VMEM((4, rows, LANES), f32),
                pltpu.VMEM((rows, LANES), f32),
                pltpu.VMEM((2, LANES, LANES), f32),
                pltpu.VMEM((3, 32, LANES), f32),
                pltpu.VMEM((9, 32, LANES), f32),
                pltpu.VMEM((9, 2, 16, LANES), f32),
                pltpu.VMEM((9, 4, 40, LANES), f32),
                pltpu.VMEM((3, 40, LANES), f32),
                pltpu.VMEM((9, 40, LANES), f32),
                pltpu.VMEM((40, LANES), f32),
                pltpu.VMEM((40, LANES), f32),
                pltpu.VMEM((ITERS - 1, 32, LANES), f32),
                pltpu.VMEM((ITERS - 1, 2, 32, LANES), f32),
                pltpu.VMEM((LANES, LANES), f32),
                pltpu.SemaphoreType.DMA((ITERS, len(FLAT))),
                pltpu.SemaphoreType.DMA((ITERS, len(FLAT))),
                pltpu.SemaphoreType.DMA((len(PANELS),)),
                pltpu.SemaphoreType.DMA((len(PANELS),)),
                pltpu.SemaphoreType.DMA((ITERS - 1, 2)),
                pltpu.SemaphoreType.DMA((ITERS - 1, 2)),
                pltpu.SemaphoreType.DMA((3,)),
            ],
            compiler_params=pltpu.CompilerParams(collective_id=0, has_side_effects=True),
        )(displace, occupied, strength)
        return pl.pallas_call(
            put_out,
            out_shape=(jax.ShapeDtypeStruct((3,) + sizes, f32), jax.ShapeDtypeStruct(sizes, f32)),
            in_specs=[vmem, vmem],
            out_specs=(pl.BlockSpec(memory_space=pl.ANY),) * 2,
            scratch_shapes=[pltpu.SemaphoreType.DMA((2,))],
        )(pltpu.with_memory_space_constraint(force, pltpu.VMEM),
          pltpu.with_memory_space_constraint(energy, pltpu.VMEM))

    in_specs = (P(None, "gx", "gy", "gz"), P("gx", "gy", "gz"), P("gx", "gy", "gz"))
    out_specs = (P(None, "gx", "gy", "gz"), P("gx", "gy", "gz"))
    return jax.shard_map(body, mesh=mesh, in_specs=in_specs, out_specs=out_specs, check_vma=False)
```

```python
import functools
import math

import jax
import jax.numpy as jnp
from jax import lax
from jax.experimental import pallas as pl
from jax.experimental.pallas import tpu as pltpu
from jax.sharding import PartitionSpec as P

ITERS = 3
RADIUS_SQ = 4.84
STEP = 0.02
AXES = ("gx", "gy", "gz")
MESH = pl.DeviceIdType.MESH
LANES = 128
DEEP = 2 * ITERS
PLANE = [(dx, dy) for dx in (-1, 0, 1) for dy in (-1, 0, 1)]
FLAT = sorted(((dx, dy, 0) for dx, dy in PLANE if (dx, dy) != (0, 0)),
              key=lambda o: (-abs(o[1]), abs(o[0]), o))
TALL = sorted(((dx, dy, dz) for dx, dy in PLANE for dz in (-1, 1)),
              key=lambda o: (-sum(abs(a) for a in o), o))
PANELS = TALL + FLAT

RADIUS = math.sqrt(RADIUS_SQ)
UNIT = 1.0 / RADIUS
RATE = -2.0 * RADIUS / math.log(2.0)
SQUARED_E = math.exp(2.0)
PULL = 2.0 / RADIUS
PUSH = 1.0 / RADIUS
FORCE = -2.0 * SQUARED_E * SQUARED_E
PAIR = 0.5 * 0.5 * SQUARED_E * SQUARED_E


def minus(o):
    return tuple(-a for a in o)


def up(rows):
    return -(-rows // 8) * 8


def low(a):
    return 0 if a == -1 else 1


def moved(value, amount, axis=1):
    amount %= value.shape[axis]
    return value if amount == 0 else pltpu.roll(value, amount, axis)


def density_sum(near, here, size):
    base = [[h - s * UNIT for s in (-1.0, 0.0, 1.0)] for h in here]
    total = jnp.zeros((size, LANES), jnp.float32)
    for dx, dy in PLANE:
        for dz in (-1, 0, 1):
            if (dx, dy, dz) == (0, 0, 0):
                continue
            sx = near(dx, dy, dz, 0) - base[0][dx + 1]
            sy = near(dx, dy, dz, 1) - base[1][dy + 1]
            sz = near(dx, dy, dz, 2) - base[2][dz + 1]
            square = sx * sx + sy * sy + sz * sz
            distance = square * lax.rsqrt(square)
            inside = 1.0 - square
            total = total + near(dx, dy, dz, 3) * (
                jnp.exp2(distance * RATE) * (inside * inside))
    return total


def force_sum(near, slope_near, here, slope, size, last):
    base = [[h - s * UNIT for s in (-1.0, 0.0, 1.0)] for h in here]
    force = [jnp.zeros((size, LANES), jnp.float32) for _ in range(3)]
    pair = jnp.zeros((size, LANES), jnp.float32)
    for dx, dy in PLANE:
        for dz in (-1, 0, 1):
            if (dx, dy, dz) == (0, 0, 0):
                continue
            sx = near(dx, dy, dz, 0) - base[0][dx + 1]
            sy = near(dx, dy, dz, 1) - base[1][dy + 1]
            sz = near(dx, dy, dz, 2) - base[2][dz + 1]
            weight = near(dx, dy, dz, 3)
            square = sx * sx + sy * sy + sz * sz
            inverse = lax.rsqrt(square)
            growth = jnp.exp2(square * inverse * RATE)
            inside = 1.0 - square
            steep = PULL + inside * inverse
            both = slope + slope_near(dx, dy, dz)
            cut = growth * inside
            scale = (both * steep + growth * (steep - PUSH)) * cut * weight
            force = [force[0] + scale * sx, force[1] + scale * sy, force[2] + scale * sz]
            if last:
                pair = pair + weight * (cut * cut)
    return force, pair


def kernel(sizes, counts, disp_hbm, occ_hbm, str_hbm, force_ref, energy_ref,
           disp_ref, occ_ref, str_ref, xs, ys, xl, yl, near, slopes, scaled,
           stage, ps, px, pz, sp, sn, ss, sscaled, sroot, xp, xq, final,
           zero, sink_xl, sink_yl, sink_px, sink_pz, sink_xq, tally,
           main_send, main_recv, panel_send, panel_recv, strip_send, strip_recv, load_sem):
    cx, cy, cz = sizes
    pitch = cy + 4
    wide = cy + 2 * DEEP
    group = cx * wide
    f32 = jnp.float32

    for src, dst in ((disp_hbm, disp_ref), (occ_hbm, occ_ref), (str_hbm, str_ref)):
        pltpu.make_async_copy(src, dst, load_sem).start()
    zero[...] = jnp.zeros(zero.shape, f32)

    def settle(rows, sem):
        part = tally.at[pl.ds(0, rows)]
        pltpu.make_async_copy(part, part, sem).wait()

    me = [lax.axis_index(axis) for axis in AXES]
    there = [[None if s == 0 else (m + s >= 0) & (m + s < n) for s in (-1, 0, 1)]
             for m, n in zip(me, counts)]

    def exists(o):
        tests = [there[a][o[a] + 1] for a in range(3) if o[a] != 0]
        return functools.reduce(lambda p, q: p & q, tests)

    def target(o):
        return {AXES[a]: me[a] + o[a] for a in range(3)}

    barrier = pltpu.get_barrier_semaphore()
    for o in PANELS:
        @pl.when(exists(o))
        def _(o=o):
            pl.semaphore_signal(barrier, inc=1, device_id=target(o), device_id_type=MESH)
    spans = [1 + (m > 0).astype(jnp.int32) + (m < n - 1).astype(jnp.int32)
             for m, n in zip(me, counts)]

    def main_rows(t, face):
        return (4 if t == 0 else 3) * cx * cy if face else up((4 if t == 0 else 3) * cx * 2)

    def transfer(o, src, spot, sink, send_sem, recv_sem):
        @pl.when(exists(o))
        def _():
            pltpu.make_async_remote_copy(
                src_ref=src, dst_ref=spot(minus(o)), send_sem=send_sem, recv_sem=recv_sem,
                device_id=target(o), device_id_type=MESH).start()

        @pl.when(jnp.logical_not(exists(o)))
        def _():
            blank = zero.at[pl.ds(0, src.shape[0])]
            pltpu.make_async_copy(blank, spot(o), recv_sem).start()
            pltpu.make_async_copy(blank, sink(o), send_sem).start()

    def main_start(t):
        for o in FLAT:
            rows = pl.ds(0, main_rows(t, o[1] == 0))
            if o[1] == 0:
                transfer(o, xs.at[t, rows], lambda n: xl.at[t, low(n[0]), rows],
                         lambda n: sink_xl.at[low(n[0]), rows], main_send, main_recv.at[t % 2])
            else:
                transfer(o, ys.at[t, low(-o[1]), rows],
                         lambda n: yl.at[t, n[0] + 1, low(n[1]), rows],
                         lambda n: sink_yl.at[n[0] + 1, low(n[1]), rows],
                         main_send, main_recv.at[t % 2])

    def main_total(t):
        return 2 * main_rows(t, True) + 6 * main_rows(t, False)

    def panel_start():
        for o in PANELS:
            j = PLANE.index
            if o[2] == 0:
                transfer(o, ps.at[1 - o[1], pl.ds(0, 32)], lambda n: px.at[j(n[:2])],
                         lambda n: sink_px.at[j(n[:2])], panel_send, panel_recv)
            else:
                transfer(o, ps.at[1 - o[1], pl.ds(8 if o[2] == -1 else 16, 16)],
                         lambda n: pz.at[j(n[:2]), low(n[2])],
                         lambda n: sink_pz.at[j(n[:2]), low(n[2])], panel_send, panel_recv)

    panel_total = 8 * 32 + 18 * 16

    def strip_start(t):
        for o in SIDES:
            transfer(o, xp.at[t], lambda n: xq.at[t, low(n[0])],
                     lambda n: sink_xq.at[low(n[0])], strip_send, strip_recv.at[t])

    SIDES = [(-1, 0, 0), (1, 0, 0)]

    settle(5 * cx * cy, load_sem)
    mine = [[disp_ref[q, x] * UNIT for x in range(cx)] for q in range(3)]
    mine.append([occ_ref[x].astype(f32) * str_ref[x] for x in range(cx)])

    def fill_sends(t):
        for q in range(4 if t == 0 else 3):
            for x in range(cx):
                i = q * cx + x
                xs[t, i * cy:(i + 1) * cy] = mine[q][x]
                ys[t, 0, i * 2:i * 2 + 2] = mine[q][x][cy - 2:cy]
                ys[t, 1, i * 2:i * 2 + 2] = mine[q][x][0:2]

    def put(q, row, piece):
        rows = piece.shape[0]
        near[0, q, row:row + rows] = moved(piece, 1)
        near[1, q, row:row + rows] = piece
        near[2, q, row:row + rows] = moved(piece, -1)

    def put_mine(t):
        for q in range(4 if t == 0 else 3):
            for x in range(cx):
                put(q, (cx + x) * pitch + 2, mine[q][x])

    def put_others(t):
        for q in range(4 if t == 0 else 3):
            for x in range(cx):
                i = q * cx + x
                for dx in (-1, 0, 1):
                    row = (cx * (dx + 1) + x) * pitch
                    if dx != 0:
                        put(q, row + 2, xl[t, low(dx), i * cy:(i + 1) * cy])
                    put(q, row, yl[t, dx + 1, 0, i * 2:i * 2 + 2])
                    put(q, row + 2 + cy, yl[t, dx + 1, 1, i * 2:i * 2 + 2])

    fill_sends(0)
    pl.semaphore_wait(barrier, spans[0] * spans[1] * spans[2] - 1)
    main_start(0)

    stage[...] = jnp.zeros(stage.shape, f32)
    tail = 3 * cx * pitch
    near[:, :, tail:] = jnp.zeros(near.shape[:2] + (near.shape[2] - tail, LANES), f32)
    sn[...] = jnp.zeros(sn.shape, f32)
    ss[...] = jnp.zeros(ss.shape, f32)

    lane = lax.broadcasted_iota(jnp.int32, (8, LANES), 1)
    half = lax.broadcasted_iota(jnp.int32, (8, LANES), 0) < 4
    column = lax.rem(lane, wide)
    for x in range(cx):
        for q in range(3):
            row = q * group + x * wide + DEEP
            stage[0, row:row + cy] = mine[q][x]
            stage[1, row:row + cy] = mine[3][x]
    turned = jnp.transpose(stage[0])
    heavy = jnp.transpose(stage[1])

    def ends_of(value):
        return (value[0:8], jnp.where(half, value[8:16], value[cz - 16:cz - 8]), value[cz - 8:cz])

    first, middle, end = ends_of(turned)
    load_first, load_middle, load_end = ends_of(heavy)
    load = jnp.where(lane < group, load_first, jnp.where(lane < 2 * group, load_middle, load_end))
    for i, piece in enumerate((middle, first, load, end)):
        ps[1, 8 * i:8 * i + 8] = piece
        ps[0, 8 * i:8 * i + 8] = jnp.where(column < DEEP, moved(piece, -cy), 0.0)
        ps[2, 8 * i:8 * i + 8] = jnp.where(column >= DEEP + cy, moved(piece, cy), 0.0)
    panel_start()
    put_mine(0)

    begin = pitch + 1
    chunk = 16
    extent = up((cx + 2) * pitch + cy + 3 - begin)

    def main_density(t):
        last = t == ITERS - 1
        settle(main_total(t), main_recv.at[t % 2])
        settle(main_total(t), main_send)
        put_others(t)
        if t == 0:
            weight = near[1, 3, begin:begin + extent]
            scaled[begin:begin + extent] = jnp.where(
                weight > 0.0, (-0.5 / SQUARED_E) / jnp.where(weight > 0.0, weight, 1.0), 0.0)
        for start in range(begin, begin + extent, chunk):
            size = min(chunk, begin + extent - start)

            def around(dx, dy, dz, q, start=start, size=size):
                row = start + dx * pitch + dy
                return near[dz + 1, q, row:row + size]

            total = 1.0 + SQUARED_E * density_sum(
                around, [near[1, q, start:start + size] for q in range(3)], size)
            root = lax.rsqrt(total)
            slope = scaled[start:start + size] * root
            slopes[0, start:start + size] = moved(slope, 1)
            slopes[1, start:start + size] = slope
            slopes[2, start:start + size] = moved(slope, -1)
            if last:
                slopes[3, start:start + size] = total * root

    def main_force(t):
        last = t == ITERS - 1
        outer = (lane < DEEP) | (lane >= cz - DEEP)

        def merge(value, q, x):
            start = group + x * wide + DEEP
            return jnp.where(outer, moved(final[start:start + cy], cz - 8 - 16 * q), value)

        for x in range(cx):
            start = (cx + x) * pitch + 2

            def around(dx, dy, dz, q, start=start):
                row = start + dx * pitch + dy
                return near[dz + 1, q, row:row + cy]

            def slope_around(dx, dy, dz, start=start):
                row = start + dx * pitch + dy
                return slopes[dz + 1, row:row + cy]

            here = [mine[q][x] for q in range(3)]
            force, pair = force_sum(around, slope_around, here, slopes[1, start:start + cy], cy, last)
            weight = mine[3][x]
            if last:
                for q in range(3):
                    force_ref[q, x] = merge((weight * FORCE) * force[q], q, x)
                energy_ref[x] = merge((weight * PAIR) * pair - jnp.where(
                    weight > 0.0, slopes[3, start:start + cy], 0.0), 3, x)
            else:
                for q in range(3):
                    mine[q][x] = here[q] + (weight * (FORCE * STEP * UNIT)) * force[q]
        if not last:
            fill_sends(t + 1)
            main_start(t + 1)
            put_mine(t + 1)

    def spread(parts, at):
        found = [moved(parts[i], group * (i - at)) for i in range(3)]
        return jnp.where(lane < group, found[0], jnp.where(
            lane < 2 * group, found[1], jnp.where(lane < 3 * group, found[2], 0.0)))

    def put_strip(q, row, value):
        for j, (dx, dy) in enumerate(PLANE):
            sp[j, q, row:row + 8] = moved(value, -(dx * wide + dy))

    def strip_step(t):
        last = t == ITERS - 1
        if t == 0:
            settle(panel_total, panel_recv)
            settle(panel_total, panel_send)

            def flat(rows):
                return [sum(ps[1, rows:rows + 8] if (dx, dy) == (0, 0)
                            else px[PLANE.index((dx, dy)), rows:rows + 8] for dy in (-1, 0, 1))
                        for dx in (-1, 0, 1)]

            def tall(side, rows):
                return [sum(pz[PLANE.index((dx, dy)), side, rows:rows + 8] for dy in (-1, 0, 1))
                        for dx in (-1, 0, 1)]

            blocks = [tall(0, 8), flat(8), flat(0), flat(24), tall(1, 0)]
            for b, parts in enumerate(blocks):
                for q in range(3):
                    put_strip(q, 8 * b, spread(parts, q))
            loads_at = flat(16)
            for b, (parts, at) in enumerate(((tall(0, 0), 2), (loads_at, 0), (loads_at, 1),
                                             (loads_at, 2), (tall(1, 8), 0))):
                weight = spread(parts, at)
                put_strip(3, 8 * b, weight)
                sscaled[8 * b:8 * b + 8] = jnp.where(
                    weight > 0.0, (-0.5 / SQUARED_E) / jnp.where(weight > 0.0, weight, 1.0), 0.0)
        else:
            settle(64, strip_recv.at[t - 1])
            settle(64, strip_send)
            for b in range(4):
                for q in range(3):
                    under = moved(xq[t - 1, 0, 8 * b:8 * b + 8], -group * q)
                    over = moved(xq[t - 1, 1, 8 * b:8 * b + 8], group * (2 - q))
                    put_strip(q, 4 + 8 * b, jnp.where(lane < group, under, jnp.where(
                        lane < 2 * group, sn[q, 4 + 8 * b:12 + 8 * b],
                        jnp.where(lane < 3 * group, over, 0.0))))

        reach = 2 * (ITERS - 1 - t)
        starts = []
        for base in (8, 32 - DEEP):
            starts += sorted({base - reach - 1, base + DEEP + reach + 1 - 8})
        for row in starts:
            def around(dx, dy, dz, q, row=row):
                return sp[PLANE.index((dx, dy)), q, row + dz:row + dz + 8]

            total = 1.0 + SQUARED_E * density_sum(
                around, [sp[4, q, row:row + 8] for q in range(3)], 8)
            root = lax.rsqrt(total)
            slope = sscaled[row:row + 8] * root
            for j, (dx, dy) in enumerate(PLANE):
                ss[j, row:row + 8] = moved(slope, -(dx * wide + dy))
            if last:
                sroot[row:row + 8] = total * root
        starts = [8, 24]
        if not last:
            starts = []
            for base in (8, 32 - DEEP):
                starts += sorted({base - reach, base + DEEP + reach - 8})
        results = []
        for row in starts:
            def around(dx, dy, dz, q, row=row):
                return sp[PLANE.index((dx, dy)), q, row + dz:row + dz + 8]

            def slope_around(dx, dy, dz, row=row):
                return ss[PLANE.index((dx, dy)), row + dz:row + dz + 8]

            here = [sp[4, q, row:row + 8] for q in range(3)]
            force, pair = force_sum(around, slope_around, here, ss[4, row:row + 8], 8, last)
            weight = sp[4, 3, row:row + 8]
            if last:
                energy = (weight * PAIR) * pair - jnp.where(
                    weight > 0.0, sroot[row:row + 8], 0.0)
                results.append([(weight * FORCE) * f for f in force] + [energy])
            else:
                for q in range(3):
                    sn[q, row:row + 8] = here[q] + (weight * (FORCE * STEP * UNIT)) * force[q]
        if not last:
            for b in range(4):
                new = [moved(sn[q, 4 + 8 * b:12 + 8 * b], group * (q - 1)) for q in range(3)]
                xp[t, 8 * b:8 * b + 8] = jnp.where(
                    lane < group, new[0], jnp.where(lane < 2 * group, new[1], new[2]))
            strip_start(t)
            return
        rows = []
        for q in range(4):
            rows += [results[1][q], results[0][q]]
        rows.append(jnp.zeros((LANES - 64, LANES), f32))
        final[...] = jnp.transpose(jnp.concatenate(rows, axis=0))

    for t in range(ITERS):
        main_density(t)
        if t < ITERS - 1:
            main_force(t)
            strip_step(t)
        else:
            strip_step(t)
            main_force(t)


def put_out(force_ref, energy_ref, force_hbm, energy_hbm, sem):
    copies = [pltpu.make_async_copy(force_ref, force_hbm, sem.at[0]),
              pltpu.make_async_copy(energy_ref, energy_hbm, sem.at[1])]
    for copy in copies:
        copy.start()
    for copy in copies:
        copy.wait()


def solution(mesh):
    counts = tuple(mesh.shape[axis] for axis in AXES)

    def body(displace, occupied, strength):
        sizes = occupied.shape
        cx, cy, cz = sizes
        assert cx == 2 and cy == 8 and cz == LANES
        pitch = cy + 4
        rows = up(2 * (pitch + 1) + up((cx + 2) * pitch + cy + 3 - (pitch + 1)))
        f32 = jnp.float32
        vmem = pl.BlockSpec(memory_space=pltpu.VMEM)
        force, energy = pl.pallas_call(
            functools.partial(kernel, sizes, counts),
            out_shape=(pltpu.VMEM((3,) + sizes, f32), pltpu.VMEM(sizes, f32)),
            in_specs=[pl.BlockSpec(memory_space=pl.ANY)] * 3,
            out_specs=(vmem, vmem),
            scratch_shapes=[
                pltpu.VMEM((3,) + sizes, f32),
                pltpu.VMEM(sizes, jnp.int32),
                pltpu.VMEM(sizes, f32),
                pltpu.VMEM((ITERS, 4 * cx * cy, LANES), f32),
                pltpu.VMEM((ITERS, 2, up(8 * cx), LANES), f32),
                pltpu.VMEM((ITERS, 2, 4 * cx * cy, LANES), f32),
                pltpu.VMEM((ITERS, 3, 2, up(8 * cx), LANES), f32),
                pltpu.VMEM((3, 4, rows, LANES), f32),
                pltpu.VMEM((4, rows, LANES), f32),
                pltpu.VMEM((rows, LANES), f32),
                pltpu.VMEM((2, LANES, LANES), f32),
                pltpu.VMEM((3, 32, LANES), f32),
                pltpu.VMEM((9, 32, LANES), f32),
                pltpu.VMEM((9, 2, 16, LANES), f32),
                pltpu.VMEM((9, 4, 40, LANES), f32),
                pltpu.VMEM((3, 40, LANES), f32),
                pltpu.VMEM((9, 40, LANES), f32),
                pltpu.VMEM((40, LANES), f32),
                pltpu.VMEM((40, LANES), f32),
                pltpu.VMEM((ITERS - 1, 32, LANES), f32),
                pltpu.VMEM((ITERS - 1, 2, 32, LANES), f32),
                pltpu.VMEM((LANES, LANES), f32),
                pltpu.VMEM((4 * cx * cy, LANES), f32),
                pltpu.VMEM((2, 4 * cx * cy, LANES), f32),
                pltpu.VMEM((3, 2, up(8 * cx), LANES), f32),
                pltpu.VMEM((9, 32, LANES), f32),
                pltpu.VMEM((9, 2, 16, LANES), f32),
                pltpu.VMEM((2, 32, LANES), f32),
                pltpu.VMEM((8 * 32 + 18 * 16, LANES), f32),
                pltpu.SemaphoreType.DMA,
                pltpu.SemaphoreType.DMA((2,)),
                pltpu.SemaphoreType.DMA,
                pltpu.SemaphoreType.DMA,
                pltpu.SemaphoreType.DMA,
                pltpu.SemaphoreType.DMA((ITERS - 1,)),
                pltpu.SemaphoreType.DMA,
            ],
            compiler_params=pltpu.CompilerParams(collective_id=0, has_side_effects=True),
        )(displace, occupied, strength)
        return pl.pallas_call(
            put_out,
            out_shape=(jax.ShapeDtypeStruct((3,) + sizes, f32), jax.ShapeDtypeStruct(sizes, f32)),
            in_specs=[vmem, vmem],
            out_specs=(pl.BlockSpec(memory_space=pl.ANY),) * 2,
            scratch_shapes=[pltpu.SemaphoreType.DMA((2,))],
        )(pltpu.with_memory_space_constraint(force, pltpu.VMEM),
          pltpu.with_memory_space_constraint(energy, pltpu.VMEM))

    in_specs = (P(None, "gx", "gy", "gz"), P("gx", "gy", "gz"), P("gx", "gy", "gz"))
    out_specs = (P(None, "gx", "gy", "gz"), P("gx", "gy", "gz"))
    return jax.shard_map(body, mesh=mesh, in_specs=in_specs, out_specs=out_specs, check_vma=False)
```

```python
import functools
import math

import jax
import jax.numpy as jnp
from jax import lax
from jax.experimental import pallas as pl
from jax.experimental.pallas import tpu as pltpu
from jax.sharding import PartitionSpec as P

ITERS = 3
RADIUS_SQ = 4.84
STEP = 0.02
AXES = ("gx", "gy", "gz")
MESH = pl.DeviceIdType.MESH
LANES = 128
DEEP = 2 * ITERS
PLANE = [(dx, dy) for dx in (-1, 0, 1) for dy in (-1, 0, 1)]
FLAT = sorted(((dx, dy, 0) for dx, dy in PLANE if (dx, dy) != (0, 0)),
              key=lambda o: (-abs(o[1]), abs(o[0]), o))
TALL = sorted(((dx, dy, dz) for dx, dy in PLANE for dz in (-1, 1)),
              key=lambda o: (-sum(abs(a) for a in o), o))
PANELS = TALL + FLAT
AROUND = [(dx, dy, dz) for dx, dy in PLANE for dz in (-1, 0, 1) if (dx, dy, dz) != (0, 0, 0)]
SIDES = [(-1, 0, 0), (1, 0, 0)]

RADIUS = math.sqrt(RADIUS_SQ)
UNIT = 1.0 / RADIUS
RATE = -2.0 * RADIUS / math.log(2.0)
SQUARED_E = math.exp(2.0)
PULL = 2.0 / RADIUS
PUSH = 1.0 / RADIUS
FORCE = -2.0 * SQUARED_E * SQUARED_E
PAIR = 0.5 * 0.5 * SQUARED_E * SQUARED_E


def minus(o):
    return tuple(-a for a in o)


def up(rows):
    return -(-rows // 8) * 8


def low(a):
    return 0 if a == -1 else 1


def moved(value, amount, axis=1):
    amount %= value.shape[axis]
    return value if amount == 0 else pltpu.roll(value, amount, axis)


def density_sum(near, here, size):
    base = [[h - s * UNIT for s in (-1.0, 0.0, 1.0)] for h in here]
    total = jnp.zeros((size, LANES), jnp.float32)
    for dx, dy in PLANE:
        for dz in (-1, 0, 1):
            if (dx, dy, dz) == (0, 0, 0):
                continue
            sx = near(dx, dy, dz, 0) - base[0][dx + 1]
            sy = near(dx, dy, dz, 1) - base[1][dy + 1]
            sz = near(dx, dy, dz, 2) - base[2][dz + 1]
            square = sx * sx + sy * sy + sz * sz
            distance = square * lax.rsqrt(square)
            inside = 1.0 - square
            total = total + near(dx, dy, dz, 3) * (
                jnp.exp2(distance * RATE) * (inside * inside))
    return total


def force_sum(near, slope_near, here, slope, size, last):
    base = [[h - s * UNIT for s in (-1.0, 0.0, 1.0)] for h in here]
    force = [jnp.zeros((size, LANES), jnp.float32) for _ in range(3)]
    pair = jnp.zeros((size, LANES), jnp.float32)
    for dx, dy in PLANE:
        for dz in (-1, 0, 1):
            if (dx, dy, dz) == (0, 0, 0):
                continue
            sx = near(dx, dy, dz, 0) - base[0][dx + 1]
            sy = near(dx, dy, dz, 1) - base[1][dy + 1]
            sz = near(dx, dy, dz, 2) - base[2][dz + 1]
            weight = near(dx, dy, dz, 3)
            square = sx * sx + sy * sy + sz * sz
            inverse = lax.rsqrt(square)
            growth = jnp.exp2(square * inverse * RATE)
            inside = 1.0 - square
            steep = PULL + inside * inverse
            both = slope + slope_near(dx, dy, dz)
            cut = growth * inside
            scale = (both * steep + growth * (steep - PUSH)) * cut * weight
            force = [force[0] + scale * sx, force[1] + scale * sy, force[2] + scale * sz]
            if last:
                pair = pair + weight * (cut * cut)
    return force, pair


def density_and_factors(near, here, factors, last):
    base = [[h - s * UNIT for s in (-1.0, 0.0, 1.0)] for h in here]
    total = jnp.zeros((8, LANES), jnp.float32)
    pair = jnp.zeros((8, LANES), jnp.float32)
    for n, (dx, dy, dz) in enumerate(AROUND):
        sx = near(dx, dy, dz, 0) - base[0][dx + 1]
        sy = near(dx, dy, dz, 1) - base[1][dy + 1]
        sz = near(dx, dy, dz, 2) - base[2][dz + 1]
        square = sx * sx + sy * sy + sz * sz
        inverse = lax.rsqrt(square)
        growth = jnp.exp2(square * inverse * RATE)
        inside = 1.0 - square
        steep = PULL + inside * inverse
        cut = growth * inside
        heavy = cut * near(dx, dy, dz, 3)
        total = total + heavy * inside
        factors[n, 0] = heavy * steep
        factors[n, 1] = heavy * (growth * (steep - PUSH))
        if last:
            pair = pair + heavy * cut
    return total, pair


def force_from_factors(near, slope_near, here, slope, factors):
    base = [[h - s * UNIT for s in (-1.0, 0.0, 1.0)] for h in here]
    force = [jnp.zeros((8, LANES), jnp.float32) for _ in range(3)]
    for n, (dx, dy, dz) in enumerate(AROUND):
        scale = (slope + slope_near(dx, dy, dz)) * factors[n, 0] + factors[n, 1]
        force = [force[q] + scale * (near(dx, dy, dz, q) - base[q][d + 1])
                 for q, d in enumerate((dx, dy, dz))]
    return force


def kernel(sizes, counts, disp_hbm, occ_hbm, str_hbm, force_ref, energy_ref,
           disp_ref, occ_ref, str_ref, xs, ys, xl, yl, near, slopes, scaled,
           stage, ps, px, pz, sp, sn, ss, sscaled, xp, xq, final,
           zero, sink_xl, sink_yl, sink_px, sink_pz, sink_xq, tally, factors, tails,
           main_send, main_recv, panel_send, panel_recv, strip_send, strip_recv, load_sem):
    cx, cy, cz = sizes
    pitch = cy + 4
    wide = cy + 2 * DEEP
    group = cx * wide
    f32 = jnp.float32

    for src, dst in ((disp_hbm, disp_ref), (occ_hbm, occ_ref), (str_hbm, str_ref)):
        pltpu.make_async_copy(src, dst, load_sem).start()
    zero[...] = jnp.zeros(zero.shape, f32)

    def settle(rows, sem):
        part = tally.at[pl.ds(0, rows)]
        pltpu.make_async_copy(part, part, sem).wait()

    me = [lax.axis_index(axis) for axis in AXES]
    there = [[None if s == 0 else (m + s >= 0) & (m + s < n) for s in (-1, 0, 1)]
             for m, n in zip(me, counts)]

    def exists(o):
        tests = [there[a][o[a] + 1] for a in range(3) if o[a] != 0]
        return functools.reduce(lambda p, q: p & q, tests)

    def target(o):
        return {AXES[a]: me[a] + o[a] for a in range(3)}

    barrier = pltpu.get_barrier_semaphore()
    for o in PANELS:
        @pl.when(exists(o))
        def _(o=o):
            pl.semaphore_signal(barrier, inc=1, device_id=target(o), device_id_type=MESH)
    spans = [1 + (m > 0).astype(jnp.int32) + (m < n - 1).astype(jnp.int32)
             for m, n in zip(me, counts)]

    def main_rows(t, face):
        return (4 if t == 0 else 3) * cx * cy if face else up((4 if t == 0 else 3) * cx * 2)

    def send(plan, send_sem, recv_sem):
        for o, src, spot, _ in plan:
            @pl.when(exists(o))
            def _(o=o, src=src, spot=spot):
                pltpu.make_async_remote_copy(
                    src_ref=src, dst_ref=spot(minus(o)), send_sem=send_sem, recv_sem=recv_sem,
                    device_id=target(o), device_id_type=MESH).start()

    def fill(plan, send_sem, recv_sem):
        for o, src, spot, sink in plan:
            @pl.when(jnp.logical_not(exists(o)))
            def _(o=o, src=src, spot=spot, sink=sink):
                blank = zero.at[pl.ds(0, src.shape[0])]
                pltpu.make_async_copy(blank, spot(o), recv_sem).start()
                pltpu.make_async_copy(blank, sink(o), send_sem).start()

    def main_plan(t):
        plan = []
        for o in FLAT:
            rows = pl.ds(0, main_rows(t, o[1] == 0))
            if o[1] == 0:
                plan.append((o, xs.at[t, rows], lambda n, r=rows: xl.at[t, low(n[0]), r],
                             lambda n, r=rows: sink_xl.at[t % 2, low(n[0]), r]))
            else:
                plan.append((o, ys.at[t, low(-o[1]), rows],
                             lambda n, r=rows: yl.at[t, n[0] + 1, low(n[1]), r],
                             lambda n, r=rows: sink_yl.at[t % 2, n[0] + 1, low(n[1]), r]))
        return plan, main_send.at[t % 2], main_recv.at[t % 2]

    def main_total(t):
        return 2 * main_rows(t, True) + 6 * main_rows(t, False)

    def panel_plan():
        plan = []
        for o in PANELS:
            if o[2] == 0:
                plan.append((o, ps.at[1 - o[1], pl.ds(0, 32)],
                             lambda n: px.at[PLANE.index(n[:2])],
                             lambda n: sink_px.at[PLANE.index(n[:2])]))
            else:
                plan.append((o, ps.at[1 - o[1], pl.ds(8 if o[2] == -1 else 16, 16)],
                             lambda n: pz.at[PLANE.index(n[:2]), low(n[2])],
                             lambda n: sink_pz.at[PLANE.index(n[:2]), low(n[2])]))
        return plan, panel_send, panel_recv

    panel_total = 8 * 32 + 18 * 16

    def strip_plan(t):
        plan = [(o, xp.at[t], lambda n: xq.at[t, low(n[0])], lambda n: sink_xq.at[t, low(n[0])])
                for o in SIDES]
        return plan, strip_send.at[t], strip_recv.at[t]


    settle(5 * cx * cy, load_sem)
    mine = [[disp_ref[q, x] * UNIT for x in range(cx)] for q in range(3)]
    mine.append([occ_ref[x].astype(f32) * str_ref[x] for x in range(cx)])

    def fill_sends(t):
        for q in range(4 if t == 0 else 3):
            for x in range(cx):
                i = q * cx + x
                xs[t, i * cy:(i + 1) * cy] = mine[q][x]
                ys[t, 0, i * 2:i * 2 + 2] = mine[q][x][cy - 2:cy]
                ys[t, 1, i * 2:i * 2 + 2] = mine[q][x][0:2]

    def put(q, row, piece):
        rows = piece.shape[0]
        near[0, q, row:row + rows] = moved(piece, 1)
        near[1, q, row:row + rows] = piece
        near[2, q, row:row + rows] = moved(piece, -1)

    def put_mine(t):
        for q in range(4 if t == 0 else 3):
            for x in range(cx):
                put(q, (cx + x) * pitch + 2, mine[q][x])

    def put_others(t):
        for q in range(4 if t == 0 else 3):
            for x in range(cx):
                i = q * cx + x
                for dx in (-1, 0, 1):
                    row = (cx * (dx + 1) + x) * pitch
                    if dx != 0:
                        put(q, row + 2, xl[t, low(dx), i * cy:(i + 1) * cy])
                    put(q, row, yl[t, dx + 1, 0, i * 2:i * 2 + 2])
                    put(q, row + 2 + cy, yl[t, dx + 1, 1, i * 2:i * 2 + 2])

    fill_sends(0)
    stage[...] = jnp.zeros(stage.shape, f32)
    tails[...] = jnp.zeros(tails.shape, f32)
    tail = 3 * cx * pitch
    near[:, :, tail:] = jnp.zeros(near.shape[:2] + (near.shape[2] - tail, LANES), f32)
    sn[...] = jnp.zeros(sn.shape, f32)
    ss[...] = jnp.zeros(ss.shape, f32)

    lane = lax.broadcasted_iota(jnp.int32, (8, LANES), 1)
    half = lax.broadcasted_iota(jnp.int32, (8, LANES), 0) < 4
    column = lax.rem(lane, wide)
    for x in range(cx):
        for q in range(3):
            row = q * group + x * wide + DEEP
            stage[0, row:row + cy] = mine[q][x]
            stage[1, row:row + cy] = mine[3][x]
    turned = jnp.transpose(stage[0])
    heavy = jnp.transpose(stage[1])

    def ends_of(value):
        return (value[0:8], jnp.where(half, value[8:16], value[cz - 16:cz - 8]), value[cz - 8:cz])

    first, middle, end = ends_of(turned)
    load_first, load_middle, load_end = ends_of(heavy)
    load = jnp.where(lane < group, load_first, jnp.where(lane < 2 * group, load_middle, load_end))
    for i, piece in enumerate((middle, first, load, end)):
        ps[1, 8 * i:8 * i + 8] = piece
        ps[0, 8 * i:8 * i + 8] = jnp.where(column < DEEP, moved(piece, -cy), 0.0)
        ps[2, 8 * i:8 * i + 8] = jnp.where(column >= DEEP + cy, moved(piece, cy), 0.0)
    for plan in (main_plan(0), panel_plan(), main_plan(1), strip_plan(0), strip_plan(1)):
        fill(*plan)
    pl.semaphore_wait(barrier, spans[0] * spans[1] * spans[2] - 1)
    send(*main_plan(0))
    send(*panel_plan())
    put_mine(0)

    begin = pitch + 1
    chunk = 16
    extent = up((cx + 2) * pitch + cy + 3 - begin)

    def main_density(t):
        last = t == ITERS - 1
        settle(main_total(t), main_recv.at[t % 2])
        settle(main_total(t), main_send.at[t % 2])
        put_others(t)
        if t == 0:
            weight = near[1, 3, begin:begin + extent]
            scaled[begin:begin + extent] = jnp.where(
                weight > 0.0, (-0.5 / SQUARED_E) / jnp.where(weight > 0.0, weight, 1.0), 0.0)
        for start in range(begin, begin + extent, chunk):
            size = min(chunk, begin + extent - start)

            def around(dx, dy, dz, q, start=start, size=size):
                row = start + dx * pitch + dy
                return near[dz + 1, q, row:row + size]

            total = 1.0 + SQUARED_E * density_sum(
                around, [near[1, q, start:start + size] for q in range(3)], size)
            root = lax.rsqrt(total)
            slope = scaled[start:start + size] * root
            slopes[0, start:start + size] = moved(slope, 1)
            slopes[1, start:start + size] = slope
            slopes[2, start:start + size] = moved(slope, -1)
            if last:
                slopes[3, start:start + size] = total * root

    def main_force(t):
        last = t == ITERS - 1
        outer = (lane < DEEP) | (lane >= cz - DEEP)

        def merge(value, q, x):
            start = group + x * wide + DEEP
            return jnp.where(outer, moved(final[start:start + cy], cz - 8 - 16 * q), value)

        for x in range(cx):
            start = (cx + x) * pitch + 2

            def around(dx, dy, dz, q, start=start):
                row = start + dx * pitch + dy
                return near[dz + 1, q, row:row + cy]

            def slope_around(dx, dy, dz, start=start):
                row = start + dx * pitch + dy
                return slopes[dz + 1, row:row + cy]

            here = [mine[q][x] for q in range(3)]
            force, pair = force_sum(around, slope_around, here, slopes[1, start:start + cy], cy, last)
            weight = mine[3][x]
            if last:
                for q in range(3):
                    force_ref[q, x] = merge((weight * FORCE) * force[q], q, x)
                energy_ref[x] = merge((weight * PAIR) * pair - jnp.where(
                    weight > 0.0, slopes[3, start:start + cy], 0.0), 3, x)
            else:
                for q in range(3):
                    mine[q][x] = here[q] + (weight * (FORCE * STEP * UNIT)) * force[q]
        if not last:
            fill_sends(t + 1)
            send(*main_plan(t + 1))
            put_mine(t + 1)

    def spread(parts, at):
        found = [moved(parts[i], group * (i - at)) for i in range(3)]
        return jnp.where(lane < group, found[0], jnp.where(
            lane < 2 * group, found[1], jnp.where(lane < 3 * group, found[2], 0.0)))

    def put_strip(q, row, value):
        for j, (dx, dy) in enumerate(PLANE):
            sp[j, q, row:row + 8] = moved(value, -(dx * wide + dy))

    def strip_step(t):
        last = t == ITERS - 1
        if t == 0:
            settle(panel_total, panel_recv)
            settle(panel_total, panel_send)

            def flat(rows):
                return [sum(ps[1, rows:rows + 8] if (dx, dy) == (0, 0)
                            else px[PLANE.index((dx, dy)), rows:rows + 8] for dy in (-1, 0, 1))
                        for dx in (-1, 0, 1)]

            def tall(side, rows):
                return [sum(pz[PLANE.index((dx, dy)), side, rows:rows + 8] for dy in (-1, 0, 1))
                        for dx in (-1, 0, 1)]

            blocks = [tall(0, 8), flat(8), flat(0), flat(24), tall(1, 0)]
            for b, parts in enumerate(blocks):
                for q in range(3):
                    put_strip(q, 8 * b, spread(parts, q))
            loads_at = flat(16)
            for b, (parts, at) in enumerate(((tall(0, 0), 2), (loads_at, 0), (loads_at, 1),
                                             (loads_at, 2), (tall(1, 8), 0))):
                weight = spread(parts, at)
                put_strip(3, 8 * b, weight)
                sscaled[8 * b:8 * b + 8] = jnp.where(
                    weight > 0.0, (-0.5 / SQUARED_E) / jnp.where(weight > 0.0, weight, 1.0), 0.0)
        else:
            settle(64, strip_recv.at[t - 1])
            settle(64, strip_send.at[t - 1])
            for b in range(4):
                for q in range(3):
                    under = moved(xq[t - 1, 0, 8 * b:8 * b + 8], -group * q)
                    over = moved(xq[t - 1, 1, 8 * b:8 * b + 8], group * (2 - q))
                    put_strip(q, 4 + 8 * b, jnp.where(lane < group, under, jnp.where(
                        lane < 2 * group, sn[q, 4 + 8 * b:12 + 8 * b],
                        jnp.where(lane < 3 * group, over, 0.0))))

        reach = 2 * (ITERS - 1 - t)
        starts = []
        for base in (8, 32 - DEEP):
            starts += sorted({base - reach - 1, base + DEEP + reach + 1 - 8})
        pairs = []
        for n, row in enumerate(starts):
            def around(dx, dy, dz, q, row=row):
                return sp[PLANE.index((dx, dy)), q, row + dz:row + dz + 8]

            total, pair = density_and_factors(
                around, [sp[4, q, row:row + 8] for q in range(3)], factors.at[n], last)
            total = 1.0 + SQUARED_E * total
            root = lax.rsqrt(total)
            slope = sscaled[row:row + 8] * root
            for j, (dx, dy) in enumerate(PLANE):
                ss[j, row:row + 8] = moved(slope, -(dx * wide + dy))
            weight = sp[4, 3, row:row + 8]
            if last:
                pairs.append((weight * PAIR) * pair - jnp.where(weight > 0.0, total * root, 0.0))
        for n, row in enumerate(starts):
            def around(dx, dy, dz, q, row=row):
                return sp[PLANE.index((dx, dy)), q, row + dz:row + dz + 8]

            def slope_around(dx, dy, dz, row=row):
                return ss[PLANE.index((dx, dy)), row + dz:row + dz + 8]

            here = [sp[4, q, row:row + 8] for q in range(3)]
            force = force_from_factors(around, slope_around, here, ss[4, row:row + 8], factors.at[n])
            weight = sp[4, 3, row:row + 8]
            if last:
                for q, value in enumerate([(weight * FORCE) * f for f in force] + [pairs[n]]):
                    tails[q, n, n:n + 8] = value
            else:
                for q in range(3):
                    sn[q, row:row + 8] = here[q] + (weight * (FORCE * STEP * UNIT)) * force[q]
        if not last:
            for b in range(4):
                new = [moved(sn[q, 4 + 8 * b:12 + 8 * b], group * (q - 1)) for q in range(3)]
                xp[t, 8 * b:8 * b + 8] = jnp.where(
                    lane < group, new[0], jnp.where(lane < 2 * group, new[1], new[2]))
            send(*strip_plan(t))
            return
        rows = []
        for q in range(4):
            rows += [tails[q, 1, 0:8], tails[q, 0, 1:9]]
        rows.append(jnp.zeros((LANES - 64, LANES), f32))
        final[...] = jnp.transpose(jnp.concatenate(rows, axis=0))

    for t in range(ITERS):
        if 0 < t < ITERS - 1:
            fill(*main_plan(t + 1))
        main_density(t)
        if t < ITERS - 1:
            main_force(t)
            strip_step(t)
        else:
            strip_step(t)
            main_force(t)


def put_out(force_ref, energy_ref, force_hbm, energy_hbm, sem):
    copies = [pltpu.make_async_copy(force_ref, force_hbm, sem.at[0]),
              pltpu.make_async_copy(energy_ref, energy_hbm, sem.at[1])]
    for copy in copies:
        copy.start()
    for copy in copies:
        copy.wait()


def solution(mesh):
    counts = tuple(mesh.shape[axis] for axis in AXES)

    def body(displace, occupied, strength):
        sizes = occupied.shape
        cx, cy, cz = sizes
        assert cx == 2 and cy == 8 and cz == LANES
        pitch = cy + 4
        rows = up(2 * (pitch + 1) + up((cx + 2) * pitch + cy + 3 - (pitch + 1)))
        f32 = jnp.float32
        vmem = pl.BlockSpec(memory_space=pltpu.VMEM)
        force, energy = pl.pallas_call(
            functools.partial(kernel, sizes, counts),
            out_shape=(pltpu.VMEM((3,) + sizes, f32), pltpu.VMEM(sizes, f32)),
            in_specs=[pl.BlockSpec(memory_space=pl.ANY)] * 3,
            out_specs=(vmem, vmem),
            scratch_shapes=[
                pltpu.VMEM((3,) + sizes, f32),
                pltpu.VMEM(sizes, jnp.int32),
                pltpu.VMEM(sizes, f32),
                pltpu.VMEM((ITERS, 4 * cx * cy, LANES), f32),
                pltpu.VMEM((ITERS, 2, up(8 * cx), LANES), f32),
                pltpu.VMEM((ITERS, 2, 4 * cx * cy, LANES), f32),
                pltpu.VMEM((ITERS, 3, 2, up(8 * cx), LANES), f32),
                pltpu.VMEM((3, 4, rows, LANES), f32),
                pltpu.VMEM((4, rows, LANES), f32),
                pltpu.VMEM((rows, LANES), f32),
                pltpu.VMEM((2, LANES, LANES), f32),
                pltpu.VMEM((3, 32, LANES), f32),
                pltpu.VMEM((9, 32, LANES), f32),
                pltpu.VMEM((9, 2, 16, LANES), f32),
                pltpu.VMEM((9, 4, 40, LANES), f32),
                pltpu.VMEM((3, 40, LANES), f32),
                pltpu.VMEM((9, 40, LANES), f32),
                pltpu.VMEM((40, LANES), f32),
                pltpu.VMEM((ITERS - 1, 32, LANES), f32),
                pltpu.VMEM((ITERS - 1, 2, 32, LANES), f32),
                pltpu.VMEM((LANES, LANES), f32),
                pltpu.VMEM((4 * cx * cy, LANES), f32),
                pltpu.VMEM((2, 2, 4 * cx * cy, LANES), f32),
                pltpu.VMEM((2, 3, 2, up(8 * cx), LANES), f32),
                pltpu.VMEM((9, 32, LANES), f32),
                pltpu.VMEM((9, 2, 16, LANES), f32),
                pltpu.VMEM((ITERS - 1, 2, 32, LANES), f32),
                pltpu.VMEM((8 * 32 + 18 * 16, LANES), f32),
                pltpu.VMEM((4, 26, 2, 8, LANES), f32),
                pltpu.VMEM((4, 2, 16, LANES), f32),
                pltpu.SemaphoreType.DMA((2,)),
                pltpu.SemaphoreType.DMA((2,)),
                pltpu.SemaphoreType.DMA,
                pltpu.SemaphoreType.DMA,
                pltpu.SemaphoreType.DMA((ITERS - 1,)),
                pltpu.SemaphoreType.DMA((ITERS - 1,)),
                pltpu.SemaphoreType.DMA,
            ],
            compiler_params=pltpu.CompilerParams(collective_id=0, has_side_effects=True),
        )(displace, occupied, strength)
        return pl.pallas_call(
            put_out,
            out_shape=(jax.ShapeDtypeStruct((3,) + sizes, f32), jax.ShapeDtypeStruct(sizes, f32)),
            in_specs=[vmem, vmem],
            out_specs=(pl.BlockSpec(memory_space=pl.ANY),) * 2,
            scratch_shapes=[pltpu.SemaphoreType.DMA((2,))],
        )(pltpu.with_memory_space_constraint(force, pltpu.VMEM),
          pltpu.with_memory_space_constraint(energy, pltpu.VMEM))

    in_specs = (P(None, "gx", "gy", "gz"), P("gx", "gy", "gz"), P("gx", "gy", "gz"))
    out_specs = (P(None, "gx", "gy", "gz"), P("gx", "gy", "gz"))
    return jax.shard_map(body, mesh=mesh, in_specs=in_specs, out_specs=out_specs, check_vma=False)
```

```python
import functools
import math

import jax
import jax.numpy as jnp
from jax import lax
from jax.experimental import pallas as pl
from jax.experimental.pallas import tpu as pltpu
from jax.sharding import PartitionSpec as P

ITERS = 3
RADIUS_SQ = 4.84
STEP = 0.02
AXES = ("gx", "gy", "gz")
MESH = pl.DeviceIdType.MESH
LANES = 128
DEEP = 2 * ITERS
PLANE = [(dx, dy) for dx in (-1, 0, 1) for dy in (-1, 0, 1)]
FLAT = sorted(((dx, dy, 0) for dx, dy in PLANE if (dx, dy) != (0, 0)),
              key=lambda o: (-abs(o[1]), abs(o[0]), o))
TALL = sorted(((dx, dy, dz) for dx, dy in PLANE for dz in (-1, 1)),
              key=lambda o: (-sum(abs(a) for a in o), o))
PANELS = TALL + FLAT
HALF = [(dx, dy, 1) for dx, dy in PLANE] + [(1, -1, 0), (1, 0, 0), (1, 1, 0), (0, 1, 0)]
AROUND = [(dx, dy, dz) for dx, dy in PLANE for dz in (-1, 0, 1) if (dx, dy, dz) != (0, 0, 0)]
SIDES = [(-1, 0, 0), (1, 0, 0)]

RADIUS = math.sqrt(RADIUS_SQ)
UNIT = 1.0 / RADIUS
RATE = -2.0 * RADIUS / math.log(2.0)
SQUARED_E = math.exp(2.0)
PULL = 2.0 / RADIUS
PUSH = 1.0 / RADIUS
FORCE = -2.0 * SQUARED_E * SQUARED_E
PAIR = 0.5 * 0.5 * SQUARED_E * SQUARED_E


def minus(o):
    return tuple(-a for a in o)


def up(rows):
    return -(-rows // 8) * 8


def low(a):
    return 0 if a == -1 else 1


def moved(value, amount, axis=1):
    amount %= value.shape[axis]
    return value if amount == 0 else pltpu.roll(value, amount, axis)


def force_sum(near, slope_near, here, slope, size, last):
    base = [[h - s * UNIT for s in (-1.0, 0.0, 1.0)] for h in here]
    force = [jnp.zeros((size, LANES), jnp.float32) for _ in range(3)]
    pair = jnp.zeros((size, LANES), jnp.float32)
    for dx, dy in PLANE:
        for dz in (-1, 0, 1):
            if (dx, dy, dz) == (0, 0, 0):
                continue
            sx = near(dx, dy, dz, 0) - base[0][dx + 1]
            sy = near(dx, dy, dz, 1) - base[1][dy + 1]
            sz = near(dx, dy, dz, 2) - base[2][dz + 1]
            weight = near(dx, dy, dz, 3)
            square = sx * sx + sy * sy + sz * sz
            inverse = lax.rsqrt(square)
            growth = jnp.exp2(square * inverse * RATE)
            inside = 1.0 - square
            steep = PULL + inside * inverse
            both = slope + slope_near(dx, dy, dz)
            cut = growth * inside
            scale = (both * steep + growth * (steep - PUSH)) * cut * weight
            force = [force[0] + scale * sx, force[1] + scale * sy, force[2] + scale * sz]
            if last:
                pair = pair + weight * (cut * cut)
    return force, pair


def density_and_factors(near, here, factors, last):
    base = [[h - s * UNIT for s in (-1.0, 0.0, 1.0)] for h in here]
    total = jnp.zeros((8, LANES), jnp.float32)
    pair = jnp.zeros((8, LANES), jnp.float32)
    for n, (dx, dy, dz) in enumerate(AROUND):
        sx = near(dx, dy, dz, 0) - base[0][dx + 1]
        sy = near(dx, dy, dz, 1) - base[1][dy + 1]
        sz = near(dx, dy, dz, 2) - base[2][dz + 1]
        square = sx * sx + sy * sy + sz * sz
        inverse = lax.rsqrt(square)
        growth = jnp.exp2(square * inverse * RATE)
        inside = 1.0 - square
        steep = PULL + inside * inverse
        cut = growth * inside
        heavy = cut * near(dx, dy, dz, 3)
        total = total + heavy * inside
        factors[n, 0] = heavy * steep
        factors[n, 1] = heavy * (growth * (steep - PUSH))
        if last:
            pair = pair + heavy * cut
    return total, pair


def force_from_factors(near, slope_near, here, slope, factors):
    base = [[h - s * UNIT for s in (-1.0, 0.0, 1.0)] for h in here]
    force = [jnp.zeros((8, LANES), jnp.float32) for _ in range(3)]
    for n, (dx, dy, dz) in enumerate(AROUND):
        scale = (slope + slope_near(dx, dy, dz)) * factors[n, 0] + factors[n, 1]
        force = [force[q] + scale * (near(dx, dy, dz, q) - base[q][d + 1])
                 for q, d in enumerate((dx, dy, dz))]
    return force


def kernel(sizes, counts, disp_hbm, occ_hbm, str_hbm, force_ref, energy_ref,
           disp_ref, occ_ref, str_ref, xs, ys, xl, yl, near, slopes, scaled, halves,
           stage, ps, px, pz, sp, sn, ss, sscaled, xp, xq, final,
           zero, sink_xl, sink_yl, sink_px, sink_pz, sink_xq, tally, factors, tails,
           main_send, main_recv, panel_send, panel_recv, strip_send, strip_recv, load_sem):
    cx, cy, cz = sizes
    pitch = cy + 4
    wide = cy + 2 * DEEP
    group = cx * wide
    f32 = jnp.float32

    for src, dst in ((disp_hbm, disp_ref), (occ_hbm, occ_ref), (str_hbm, str_ref)):
        pltpu.make_async_copy(src, dst, load_sem).start()
    zero[...] = jnp.zeros(zero.shape, f32)

    def settle(rows, sem):
        part = tally.at[pl.ds(0, rows)]
        pltpu.make_async_copy(part, part, sem).wait()

    me = [lax.axis_index(axis) for axis in AXES]
    there = [[None if s == 0 else (m + s >= 0) & (m + s < n) for s in (-1, 0, 1)]
             for m, n in zip(me, counts)]

    def exists(o):
        tests = [there[a][o[a] + 1] for a in range(3) if o[a] != 0]
        return functools.reduce(lambda p, q: p & q, tests)

    def target(o):
        return {AXES[a]: me[a] + o[a] for a in range(3)}

    barrier = pltpu.get_barrier_semaphore()
    for o in PANELS:
        @pl.when(exists(o))
        def _(o=o):
            pl.semaphore_signal(barrier, inc=1, device_id=target(o), device_id_type=MESH)
    spans = [1 + (m > 0).astype(jnp.int32) + (m < n - 1).astype(jnp.int32)
             for m, n in zip(me, counts)]

    def main_rows(t, face):
        return (4 if t == 0 else 3) * cx * cy if face else up((4 if t == 0 else 3) * cx * 2)

    def send(plan, send_sem, recv_sem):
        for o, src, spot, _ in plan:
            @pl.when(exists(o))
            def _(o=o, src=src, spot=spot):
                pltpu.make_async_remote_copy(
                    src_ref=src, dst_ref=spot(minus(o)), send_sem=send_sem, recv_sem=recv_sem,
                    device_id=target(o), device_id_type=MESH).start()

    def fill(plan, send_sem, recv_sem):
        for o, src, spot, sink in plan:
            @pl.when(jnp.logical_not(exists(o)))
            def _(o=o, src=src, spot=spot, sink=sink):
                blank = zero.at[pl.ds(0, src.shape[0])]
                pltpu.make_async_copy(blank, spot(o), recv_sem).start()
                pltpu.make_async_copy(blank, sink(o), send_sem).start()

    def main_plan(t):
        plan = []
        for o in FLAT:
            rows = pl.ds(0, main_rows(t, o[1] == 0))
            if o[1] == 0:
                plan.append((o, xs.at[t, rows], lambda n, r=rows: xl.at[t, low(n[0]), r],
                             lambda n, r=rows: sink_xl.at[t % 2, low(n[0]), r]))
            else:
                plan.append((o, ys.at[t, low(-o[1]), rows],
                             lambda n, r=rows: yl.at[t, n[0] + 1, low(n[1]), r],
                             lambda n, r=rows: sink_yl.at[t % 2, n[0] + 1, low(n[1]), r]))
        return plan, main_send.at[t % 2], main_recv.at[t % 2]

    def main_total(t):
        return 2 * main_rows(t, True) + 6 * main_rows(t, False)

    def panel_plan():
        plan = []
        for o in PANELS:
            if o[2] == 0:
                plan.append((o, ps.at[1 - o[1], pl.ds(0, 32)],
                             lambda n: px.at[PLANE.index(n[:2])],
                             lambda n: sink_px.at[PLANE.index(n[:2])]))
            else:
                plan.append((o, ps.at[1 - o[1], pl.ds(8 if o[2] == -1 else 16, 16)],
                             lambda n: pz.at[PLANE.index(n[:2]), low(n[2])],
                             lambda n: sink_pz.at[PLANE.index(n[:2]), low(n[2])]))
        return plan, panel_send, panel_recv

    panel_total = 8 * 32 + 18 * 16

    def strip_plan(t):
        plan = [(o, xp.at[t], lambda n: xq.at[t, low(n[0])], lambda n: sink_xq.at[t, low(n[0])])
                for o in SIDES]
        return plan, strip_send.at[t], strip_recv.at[t]


    settle(5 * cx * cy, load_sem)
    mine = [[disp_ref[q, x] * UNIT for x in range(cx)] for q in range(3)]
    mine.append([occ_ref[x].astype(f32) * str_ref[x] for x in range(cx)])

    def fill_sends(t):
        for q in range(4 if t == 0 else 3):
            for x in range(cx):
                i = q * cx + x
                xs[t, i * cy:(i + 1) * cy] = mine[q][x]
                ys[t, 0, i * 2:i * 2 + 2] = mine[q][x][cy - 2:cy]
                ys[t, 1, i * 2:i * 2 + 2] = mine[q][x][0:2]

    def put(q, row, piece):
        rows = piece.shape[0]
        near[0, q, row:row + rows] = moved(piece, 1)
        near[1, q, row:row + rows] = piece
        near[2, q, row:row + rows] = moved(piece, -1)

    def put_mine(t):
        for q in range(4 if t == 0 else 3):
            for x in range(cx):
                put(q, (cx + x) * pitch + 2, mine[q][x])

    def put_others(t):
        for q in range(4 if t == 0 else 3):
            for x in range(cx):
                i = q * cx + x
                for dx in (-1, 0, 1):
                    row = (cx * (dx + 1) + x) * pitch
                    if dx != 0:
                        put(q, row + 2, xl[t, low(dx), i * cy:(i + 1) * cy])
                    put(q, row, yl[t, dx + 1, 0, i * 2:i * 2 + 2])
                    put(q, row + 2 + cy, yl[t, dx + 1, 1, i * 2:i * 2 + 2])

    fill_sends(0)
    pl.semaphore_wait(barrier, spans[0] * spans[1] * spans[2] - 1)
    send(*main_plan(0))
    fill(*main_plan(0))
    stage[...] = jnp.zeros(stage.shape, f32)
    tails[...] = jnp.zeros(tails.shape, f32)
    tail = 3 * cx * pitch
    near[:, :, tail:] = jnp.zeros(near.shape[:2] + (near.shape[2] - tail, LANES), f32)
    sn[...] = jnp.zeros(sn.shape, f32)
    ss[...] = jnp.zeros(ss.shape, f32)

    lane = lax.broadcasted_iota(jnp.int32, (8, LANES), 1)
    half = lax.broadcasted_iota(jnp.int32, (8, LANES), 0) < 4
    column = lax.rem(lane, wide)
    for x in range(cx):
        for q in range(3):
            row = q * group + x * wide + DEEP
            stage[0, row:row + cy] = mine[q][x]
            stage[1, row:row + cy] = mine[3][x]
    turned = jnp.transpose(stage[0])
    heavy = jnp.transpose(stage[1])

    def ends_of(value):
        return (value[0:8], jnp.where(half, value[8:16], value[cz - 16:cz - 8]), value[cz - 8:cz])

    first, middle, end = ends_of(turned)
    load_first, load_middle, load_end = ends_of(heavy)
    load = jnp.where(lane < group, load_first, jnp.where(lane < 2 * group, load_middle, load_end))
    for i, piece in enumerate((middle, first, load, end)):
        ps[1, 8 * i:8 * i + 8] = piece
        ps[0, 8 * i:8 * i + 8] = jnp.where(column < DEEP, moved(piece, -cy), 0.0)
        ps[2, 8 * i:8 * i + 8] = jnp.where(column >= DEEP + cy, moved(piece, cy), 0.0)
    send(*panel_plan())
    fill(*panel_plan())
    put_mine(0)
    fill(*main_plan(1))

    begin = pitch + 1
    extent = up((cx + 2) * pitch + cy + 3 - begin)

    def main_arrive(t):
        settle(main_total(t), main_recv.at[t % 2])
        settle(main_total(t), main_send.at[t % 2])
        put_others(t)
        if t == 0:
            weight = near[1, 3, begin:begin + extent]
            scaled[begin:begin + extent] = jnp.where(
                weight > 0.0, (-0.5 / SQUARED_E) / jnp.where(weight > 0.0, weight, 1.0), 0.0)

    last_row = begin + (cx + 2) * pitch - 3

    def pair_values(n):
        dx, dy, dz = HALF[n]
        shift = dx * pitch + dy
        for start in range(begin - max(shift, 0), last_row + 1 - min(shift, 0), 8):
            parts = []
            for q, d in enumerate((dx, dy, dz)):
                far = near[dz + 1, q, start + shift:start + shift + 8]
                parts.append(far - (near[1, q, start:start + 8] - d * UNIT))
            square = parts[0] * parts[0] + parts[1] * parts[1] + parts[2] * parts[2]
            inside = 1.0 - square
            halves[n, start:start + 8] = jnp.exp2(square * lax.rsqrt(square) * RATE) * (inside * inside)

    def main_density(t):
        last = t == ITERS - 1
        for n in range(len(HALF)):
            pair_values(n)
        for start in range(begin, last_row + 1, 8):
            total = jnp.zeros((8, LANES), f32)
            behind = jnp.zeros((8, LANES), f32)
            for n, (dx, dy, dz) in enumerate(HALF):
                to = start + dx * pitch + dy
                back = start - dx * pitch - dy
                total = total + near[dz + 1, 3, to:to + 8] * halves[n, start:start + 8]
                reaction = near[1, 3, back:back + 8] * halves[n, back:back + 8]
                if dz == 0:
                    total = total + reaction
                else:
                    behind = behind + reaction
            total = 1.0 + SQUARED_E * (total + moved(behind, 1))
            root = lax.rsqrt(total)
            slope = scaled[start:start + 8] * root
            slopes[0, start:start + 8] = moved(slope, 1)
            slopes[1, start:start + 8] = slope
            slopes[2, start:start + 8] = moved(slope, -1)
            if last:
                slopes[3, start:start + 8] = total * root

    def main_force(t, slabs):
        last = t == ITERS - 1
        values = []
        for x in slabs:
            start = (cx + x) * pitch + 2

            def around(dx, dy, dz, q, start=start):
                row = start + dx * pitch + dy
                return near[dz + 1, q, row:row + cy]

            def slope_around(dx, dy, dz, start=start):
                row = start + dx * pitch + dy
                return slopes[dz + 1, row:row + cy]

            here = [mine[q][x] for q in range(3)]
            force, pair = force_sum(around, slope_around, here, slopes[1, start:start + cy], cy, last)
            weight = mine[3][x]
            if last:
                values.append([(weight * FORCE) * f for f in force] + [
                    (weight * PAIR) * pair - jnp.where(weight > 0.0, slopes[3, start:start + cy], 0.0)])
            else:
                for q in range(3):
                    mine[q][x] = here[q] + (weight * (FORCE * STEP * UNIT)) * force[q]
        return values

    def main_send_next(t):
        fill_sends(t + 1)
        send(*main_plan(t + 1))
        put_mine(t + 1)

    def merge(values):
        outer = (lane < DEEP) | (lane >= cz - DEEP)
        for x in range(cx):
            start = group + x * wide + DEEP
            for q in range(4):
                spot = force_ref.at[q, x] if q < 3 else energy_ref.at[x]
                spot[...] = jnp.where(outer, moved(final[start:start + cy], cz - 8 - 16 * q), values[x][q])

    def spread(parts, at):
        found = [moved(parts[i], group * (i - at)) for i in range(3)]
        return jnp.where(lane < group, found[0], jnp.where(
            lane < 2 * group, found[1], jnp.where(lane < 3 * group, found[2], 0.0)))

    def put_strip(q, row, value):
        for j, (dx, dy) in enumerate(PLANE):
            sp[j, q, row:row + 8] = moved(value, -(dx * wide + dy))

    def strip_arrive(t):
        if t == 0:
            settle(panel_total, panel_recv)
            settle(panel_total, panel_send)

            def flat(rows):
                return [sum(ps[1, rows:rows + 8] if (dx, dy) == (0, 0)
                            else px[PLANE.index((dx, dy)), rows:rows + 8] for dy in (-1, 0, 1))
                        for dx in (-1, 0, 1)]

            def tall(side, rows):
                return [sum(pz[PLANE.index((dx, dy)), side, rows:rows + 8] for dy in (-1, 0, 1))
                        for dx in (-1, 0, 1)]

            blocks = [tall(0, 8), flat(8), flat(0), flat(24), tall(1, 0)]
            for b, parts in enumerate(blocks):
                for q in range(3):
                    put_strip(q, 8 * b, spread(parts, q))
            loads_at = flat(16)
            for b, (parts, at) in enumerate(((tall(0, 0), 2), (loads_at, 0), (loads_at, 1),
                                             (loads_at, 2), (tall(1, 8), 0))):
                weight = spread(parts, at)
                put_strip(3, 8 * b, weight)
                sscaled[8 * b:8 * b + 8] = jnp.where(
                    weight > 0.0, (-0.5 / SQUARED_E) / jnp.where(weight > 0.0, weight, 1.0), 0.0)
        else:
            settle(64, strip_recv.at[t - 1])
            settle(64, strip_send.at[t - 1])
            for b in range(4):
                for q in range(3):
                    under = moved(xq[t - 1, 0, 8 * b:8 * b + 8], -group * q)
                    over = moved(xq[t - 1, 1, 8 * b:8 * b + 8], group * (2 - q))
                    put_strip(q, 4 + 8 * b, jnp.where(lane < group, under, jnp.where(
                        lane < 2 * group, sn[q, 4 + 8 * b:12 + 8 * b],
                        jnp.where(lane < 3 * group, over, 0.0))))


    def strip_density(t):
        last = t == ITERS - 1
        reach = 2 * (ITERS - 1 - t)
        starts = []
        for base in (8, 32 - DEEP):
            starts += sorted({base - reach - 1, base + DEEP + reach + 1 - 8})
        pairs = []
        for n, row in enumerate(starts):
            def around(dx, dy, dz, q, row=row):
                return sp[PLANE.index((dx, dy)), q, row + dz:row + dz + 8]

            total, pair = density_and_factors(
                around, [sp[4, q, row:row + 8] for q in range(3)], factors.at[n], last)
            total = 1.0 + SQUARED_E * total
            root = lax.rsqrt(total)
            slope = sscaled[row:row + 8] * root
            for j, (dx, dy) in enumerate(PLANE):
                ss[j, row:row + 8] = moved(slope, -(dx * wide + dy))
            weight = sp[4, 3, row:row + 8]
            if last:
                pairs.append((weight * PAIR) * pair - jnp.where(weight > 0.0, total * root, 0.0))
        return starts, pairs

    def strip_force(t, starts, pairs):
        last = t == ITERS - 1
        for n, row in enumerate(starts):
            def around(dx, dy, dz, q, row=row):
                return sp[PLANE.index((dx, dy)), q, row + dz:row + dz + 8]

            def slope_around(dx, dy, dz, row=row):
                return ss[PLANE.index((dx, dy)), row + dz:row + dz + 8]

            here = [sp[4, q, row:row + 8] for q in range(3)]
            force = force_from_factors(around, slope_around, here, ss[4, row:row + 8], factors.at[n])
            weight = sp[4, 3, row:row + 8]
            if last:
                for q, value in enumerate([(weight * FORCE) * f for f in force] + [pairs[n]]):
                    tails[q, n, n:n + 8] = value
            else:
                for q in range(3):
                    sn[q, row:row + 8] = here[q] + (weight * (FORCE * STEP * UNIT)) * force[q]
        if not last:
            for b in range(4):
                new = [moved(sn[q, 4 + 8 * b:12 + 8 * b], group * (q - 1)) for q in range(3)]
                xp[t, 8 * b:8 * b + 8] = jnp.where(
                    lane < group, new[0], jnp.where(lane < 2 * group, new[1], new[2]))
            send(*strip_plan(t))
            return
        rows = []
        for q in range(4):
            rows += [tails[q, 1, 0:8], tails[q, 0, 1:9]]
        rows.append(jnp.zeros((LANES - 64, LANES), f32))
        final[...] = jnp.transpose(jnp.concatenate(rows, axis=0))

    for t in range(ITERS):
        main_arrive(t)
        if t < ITERS - 1:
            main_density(t)
            main_force(t, range(cx))
            main_send_next(t)
            strip_arrive(t)
            strip_force(t, *strip_density(t))
            fill(*strip_plan(t))
            if t + 2 < ITERS:
                fill(*main_plan(t + 2))
        else:
            main_density(t)
            strip_arrive(t)
            strips = strip_density(t)
            values = main_force(t, [0])
            strip_force(t, *strips)
            merge(values + main_force(t, range(1, cx)))


def put_out(force_ref, energy_ref, force_hbm, energy_hbm, sem):
    copies = [pltpu.make_async_copy(force_ref, force_hbm, sem.at[0]),
              pltpu.make_async_copy(energy_ref, energy_hbm, sem.at[1])]
    for copy in copies:
        copy.start()
    for copy in copies:
        copy.wait()


def solution(mesh):
    counts = tuple(mesh.shape[axis] for axis in AXES)

    def body(displace, occupied, strength):
        sizes = occupied.shape
        cx, cy, cz = sizes
        assert cx == 2 and cy == 8 and cz == LANES
        pitch = cy + 4
        rows = up(2 * (pitch + 1) + up((cx + 2) * pitch + cy + 3 - (pitch + 1)))
        f32 = jnp.float32
        vmem = pl.BlockSpec(memory_space=pltpu.VMEM)
        force, energy = pl.pallas_call(
            functools.partial(kernel, sizes, counts),
            out_shape=(pltpu.VMEM((3,) + sizes, f32), pltpu.VMEM(sizes, f32)),
            in_specs=[pl.BlockSpec(memory_space=pl.ANY)] * 3,
            out_specs=(vmem, vmem),
            scratch_shapes=[
                pltpu.VMEM((3,) + sizes, f32),
                pltpu.VMEM(sizes, jnp.int32),
                pltpu.VMEM(sizes, f32),
                pltpu.VMEM((ITERS, 4 * cx * cy, LANES), f32),
                pltpu.VMEM((ITERS, 2, up(8 * cx), LANES), f32),
                pltpu.VMEM((ITERS, 2, 4 * cx * cy, LANES), f32),
                pltpu.VMEM((ITERS, 3, 2, up(8 * cx), LANES), f32),
                pltpu.VMEM((3, 4, rows, LANES), f32),
                pltpu.VMEM((4, rows, LANES), f32),
                pltpu.VMEM((rows, LANES), f32),
                pltpu.VMEM((len(HALF), rows, LANES), f32),
                pltpu.VMEM((2, LANES, LANES), f32),
                pltpu.VMEM((3, 32, LANES), f32),
                pltpu.VMEM((9, 32, LANES), f32),
                pltpu.VMEM((9, 2, 16, LANES), f32),
                pltpu.VMEM((9, 4, 40, LANES), f32),
                pltpu.VMEM((3, 40, LANES), f32),
                pltpu.VMEM((9, 40, LANES), f32),
                pltpu.VMEM((40, LANES), f32),
                pltpu.VMEM((ITERS - 1, 32, LANES), f32),
                pltpu.VMEM((ITERS - 1, 2, 32, LANES), f32),
                pltpu.VMEM((LANES, LANES), f32),
                pltpu.VMEM((4 * cx * cy, LANES), f32),
                pltpu.VMEM((2, 2, 4 * cx * cy, LANES), f32),
                pltpu.VMEM((2, 3, 2, up(8 * cx), LANES), f32),
                pltpu.VMEM((9, 32, LANES), f32),
                pltpu.VMEM((9, 2, 16, LANES), f32),
                pltpu.VMEM((ITERS - 1, 2, 32, LANES), f32),
                pltpu.VMEM((8 * 32 + 18 * 16, LANES), f32),
                pltpu.VMEM((4, 26, 2, 8, LANES), f32),
                pltpu.VMEM((4, 2, 16, LANES), f32),
                pltpu.SemaphoreType.DMA((2,)),
                pltpu.SemaphoreType.DMA((2,)),
                pltpu.SemaphoreType.DMA,
                pltpu.SemaphoreType.DMA,
                pltpu.SemaphoreType.DMA((ITERS - 1,)),
                pltpu.SemaphoreType.DMA((ITERS - 1,)),
                pltpu.SemaphoreType.DMA,
            ],
            compiler_params=pltpu.CompilerParams(collective_id=0, has_side_effects=True),
        )(displace, occupied, strength)
        return pl.pallas_call(
            put_out,
            out_shape=(jax.ShapeDtypeStruct((3,) + sizes, f32), jax.ShapeDtypeStruct(sizes, f32)),
            in_specs=[vmem, vmem],
            out_specs=(pl.BlockSpec(memory_space=pl.ANY),) * 2,
            scratch_shapes=[pltpu.SemaphoreType.DMA((2,))],
        )(pltpu.with_memory_space_constraint(force, pltpu.VMEM),
          pltpu.with_memory_space_constraint(energy, pltpu.VMEM))

    in_specs = (P(None, "gx", "gy", "gz"), P("gx", "gy", "gz"), P("gx", "gy", "gz"))
    out_specs = (P(None, "gx", "gy", "gz"), P("gx", "gy", "gz"))
    return jax.shard_map(body, mesh=mesh, in_specs=in_specs, out_specs=out_specs, check_vma=False)
```

```python
import functools
import math

import jax
import jax.numpy as jnp
from jax import lax
from jax.experimental import pallas as pl
from jax.experimental.pallas import tpu as pltpu
from jax.sharding import PartitionSpec as P

ITERS = 3
RADIUS_SQ = 4.84
STEP = 0.02
AXES = ("gx", "gy", "gz")
MESH = pl.DeviceIdType.MESH
LANES = 128
DEEP = 2 * ITERS
PLANE = [(dx, dy) for dx in (-1, 0, 1) for dy in (-1, 0, 1)]
FLAT = sorted(((dx, dy, 0) for dx, dy in PLANE if (dx, dy) != (0, 0)),
              key=lambda o: (-abs(o[1]), abs(o[0]), o))
TALL = sorted(((dx, dy, dz) for dx, dy in PLANE for dz in (-1, 1)),
              key=lambda o: (-sum(abs(a) for a in o), o))
PANELS = TALL + FLAT
HALF = [(dx, dy, 1) for dx, dy in PLANE] + [(1, -1, 0), (1, 0, 0), (1, 1, 0), (0, 1, 0)]
AROUND = [(dx, dy, dz) for dx, dy in PLANE for dz in (-1, 0, 1) if (dx, dy, dz) != (0, 0, 0)]
SIDES = [(-1, 0, 0), (1, 0, 0)]

RADIUS = math.sqrt(RADIUS_SQ)
UNIT = 1.0 / RADIUS
RATE = -2.0 * RADIUS / math.log(2.0)
SQUARED_E = math.exp(2.0)
PULL = 2.0 / RADIUS
PUSH = 1.0 / RADIUS
FORCE = -2.0 * SQUARED_E * SQUARED_E
PAIR = 0.5 * 0.5 * SQUARED_E * SQUARED_E


def minus(o):
    return tuple(-a for a in o)


def up(rows):
    return -(-rows // 8) * 8


def low(a):
    return 0 if a == -1 else 1


def moved(value, amount, axis=1):
    amount %= value.shape[axis]
    return value if amount == 0 else pltpu.roll(value, amount, axis)


def density_and_factors(near, here, factors, last):
    base = [[h - s * UNIT for s in (-1.0, 0.0, 1.0)] for h in here]
    total = jnp.zeros((8, LANES), jnp.float32)
    pair = jnp.zeros((8, LANES), jnp.float32)
    for n, (dx, dy, dz) in enumerate(AROUND):
        sx = near(dx, dy, dz, 0) - base[0][dx + 1]
        sy = near(dx, dy, dz, 1) - base[1][dy + 1]
        sz = near(dx, dy, dz, 2) - base[2][dz + 1]
        square = sx * sx + sy * sy + sz * sz
        inverse = lax.rsqrt(square)
        growth = jnp.exp2(square * inverse * RATE)
        inside = 1.0 - square
        steep = PULL + inside * inverse
        cut = growth * inside
        heavy = cut * near(dx, dy, dz, 3)
        total = total + heavy * inside
        factors[n, 0] = heavy * steep
        factors[n, 1] = heavy * (growth * (steep - PUSH))
        if last:
            pair = pair + heavy * cut
    return total, pair


def force_from_factors(near, slope_near, here, slope, factors):
    base = [[h - s * UNIT for s in (-1.0, 0.0, 1.0)] for h in here]
    force = [jnp.zeros((8, LANES), jnp.float32) for _ in range(3)]
    for n, (dx, dy, dz) in enumerate(AROUND):
        scale = (slope + slope_near(dx, dy, dz)) * factors[n, 0] + factors[n, 1]
        force = [force[q] + scale * (near(dx, dy, dz, q) - base[q][d + 1])
                 for q, d in enumerate((dx, dy, dz))]
    return force


def kernel(sizes, counts, disp_hbm, occ_hbm, str_hbm, force_ref, energy_ref,
           disp_ref, occ_ref, str_ref, xs, ys, xl, yl, near, slopes, scaled, halves, bonds,
           stage, ps, px, pz, sp, sn, ss, sscaled, xp, xq, final,
           zero, sink_xl, sink_yl, sink_px, sink_pz, sink_xq, tally, factors, tails,
           main_send, main_recv, panel_send, panel_recv, strip_send, strip_recv, load_sem):
    cx, cy, cz = sizes
    pitch = cy + 4
    wide = cy + 2 * DEEP
    group = cx * wide
    f32 = jnp.float32

    for src, dst in ((disp_hbm, disp_ref), (occ_hbm, occ_ref), (str_hbm, str_ref)):
        pltpu.make_async_copy(src, dst, load_sem).start()
    zero[...] = jnp.zeros(zero.shape, f32)

    def settle(rows, sem):
        part = tally.at[pl.ds(0, rows)]
        pltpu.make_async_copy(part, part, sem).wait()

    me = [lax.axis_index(axis) for axis in AXES]
    there = [[None if s == 0 else (m + s >= 0) & (m + s < n) for s in (-1, 0, 1)]
             for m, n in zip(me, counts)]

    def exists(o):
        tests = [there[a][o[a] + 1] for a in range(3) if o[a] != 0]
        return functools.reduce(lambda p, q: p & q, tests)

    def target(o):
        return {AXES[a]: me[a] + o[a] for a in range(3)}

    barrier = pltpu.get_barrier_semaphore()
    for o in PANELS:
        @pl.when(exists(o))
        def _(o=o):
            pl.semaphore_signal(barrier, inc=1, device_id=target(o), device_id_type=MESH)
    spans = [1 + (m > 0).astype(jnp.int32) + (m < n - 1).astype(jnp.int32)
             for m, n in zip(me, counts)]

    def main_rows(t, face):
        return (4 if t == 0 else 3) * cx * cy if face else up((4 if t == 0 else 3) * cx * 2)

    def send(plan, send_sem, recv_sem):
        for o, src, spot, _ in plan:
            @pl.when(exists(o))
            def _(o=o, src=src, spot=spot):
                pltpu.make_async_remote_copy(
                    src_ref=src, dst_ref=spot(minus(o)), send_sem=send_sem, recv_sem=recv_sem,
                    device_id=target(o), device_id_type=MESH).start()

    def fill(plan, send_sem, recv_sem):
        for o, src, spot, sink in plan:
            @pl.when(jnp.logical_not(exists(o)))
            def _(o=o, src=src, spot=spot, sink=sink):
                blank = zero.at[pl.ds(0, src.shape[0])]
                pltpu.make_async_copy(blank, spot(o), recv_sem).start()
                pltpu.make_async_copy(blank, sink(o), send_sem).start()

    def main_plan(t):
        plan = []
        for o in FLAT:
            rows = pl.ds(0, main_rows(t, o[1] == 0))
            if o[1] == 0:
                plan.append((o, xs.at[t, rows], lambda n, r=rows: xl.at[t, low(n[0]), r],
                             lambda n, r=rows: sink_xl.at[t % 2, low(n[0]), r]))
            else:
                plan.append((o, ys.at[t, low(-o[1]), rows],
                             lambda n, r=rows: yl.at[t, n[0] + 1, low(n[1]), r],
                             lambda n, r=rows: sink_yl.at[t % 2, n[0] + 1, low(n[1]), r]))
        return plan, main_send.at[t % 2], main_recv.at[t % 2]

    def main_total(t):
        return 2 * main_rows(t, True) + 6 * main_rows(t, False)

    def panel_plan():
        plan = []
        for o in PANELS:
            if o[2] == 0:
                plan.append((o, ps.at[1 - o[1], pl.ds(0, 32)],
                             lambda n: px.at[PLANE.index(n[:2])],
                             lambda n: sink_px.at[PLANE.index(n[:2])]))
            else:
                plan.append((o, ps.at[1 - o[1], pl.ds(8 if o[2] == -1 else 16, 16)],
                             lambda n: pz.at[PLANE.index(n[:2]), low(n[2])],
                             lambda n: sink_pz.at[PLANE.index(n[:2]), low(n[2])]))
        return plan, panel_send, panel_recv

    panel_total = 8 * 32 + 18 * 16

    def strip_plan(t):
        plan = [(o, xp.at[t], lambda n: xq.at[t, low(n[0])], lambda n: sink_xq.at[t, low(n[0])])
                for o in SIDES]
        return plan, strip_send.at[t], strip_recv.at[t]


    settle(5 * cx * cy, load_sem)
    mine = [[disp_ref[q, x] * UNIT for x in range(cx)] for q in range(3)]
    mine.append([occ_ref[x].astype(f32) * str_ref[x] for x in range(cx)])

    def fill_sends(t):
        for q in range(4 if t == 0 else 3):
            for x in range(cx):
                i = q * cx + x
                xs[t, i * cy:(i + 1) * cy] = mine[q][x]
                ys[t, 0, i * 2:i * 2 + 2] = mine[q][x][cy - 2:cy]
                ys[t, 1, i * 2:i * 2 + 2] = mine[q][x][0:2]

    def put(q, row, piece):
        rows = piece.shape[0]
        near[0, q, row:row + rows] = moved(piece, 1)
        near[1, q, row:row + rows] = piece
        near[2, q, row:row + rows] = moved(piece, -1)

    def put_mine(t):
        for q in range(4 if t == 0 else 3):
            for x in range(cx):
                put(q, (cx + x) * pitch + 2, mine[q][x])

    def put_others(t):
        for q in range(4 if t == 0 else 3):
            for x in range(cx):
                i = q * cx + x
                for dx in (-1, 0, 1):
                    row = (cx * (dx + 1) + x) * pitch
                    if dx != 0:
                        put(q, row + 2, xl[t, low(dx), i * cy:(i + 1) * cy])
                    put(q, row, yl[t, dx + 1, 0, i * 2:i * 2 + 2])
                    put(q, row + 2 + cy, yl[t, dx + 1, 1, i * 2:i * 2 + 2])

    fill_sends(0)
    stage[...] = jnp.zeros(stage.shape, f32)

    lane = lax.broadcasted_iota(jnp.int32, (8, LANES), 1)
    half = lax.broadcasted_iota(jnp.int32, (8, LANES), 0) < 4
    column = lax.rem(lane, wide)
    for x in range(cx):
        for q in range(3):
            row = q * group + x * wide + DEEP
            stage[0, row:row + cy] = mine[q][x]
            stage[1, row:row + cy] = mine[3][x]
    turned = jnp.transpose(stage[0])
    heavy = jnp.transpose(stage[1])

    def ends_of(value):
        return (value[0:8], jnp.where(half, value[8:16], value[cz - 16:cz - 8]), value[cz - 8:cz])

    first, middle, end = ends_of(turned)
    load_first, load_middle, load_end = ends_of(heavy)
    load = jnp.where(lane < group, load_first, jnp.where(lane < 2 * group, load_middle, load_end))
    for i, piece in enumerate((middle, first, load, end)):
        ps[1, 8 * i:8 * i + 8] = piece
        ps[0, 8 * i:8 * i + 8] = jnp.where(column < DEEP, moved(piece, -cy), 0.0)
        ps[2, 8 * i:8 * i + 8] = jnp.where(column >= DEEP + cy, moved(piece, cy), 0.0)
    pl.semaphore_wait(barrier, spans[0] * spans[1] * spans[2] - 1)
    send(*main_plan(0))
    send(*panel_plan())
    fill(*main_plan(0))
    fill(*panel_plan())
    tails[...] = jnp.zeros(tails.shape, f32)
    tail = 3 * cx * pitch
    near[:, :, tail:] = jnp.zeros(near.shape[:2] + (near.shape[2] - tail, LANES), f32)
    sn[...] = jnp.zeros(sn.shape, f32)
    ss[...] = jnp.zeros(ss.shape, f32)
    put_mine(0)
    fill(*main_plan(1))

    begin = pitch + 1
    extent = up((cx + 2) * pitch + cy + 3 - begin)

    def main_arrive(t):
        settle(main_total(t), main_recv.at[t % 2])
        settle(main_total(t), main_send.at[t % 2])
        put_others(t)
        if t == 0:
            weight = near[1, 3, begin:begin + extent]
            scaled[begin:begin + extent] = jnp.where(
                weight > 0.0, (-0.5 / SQUARED_E) / jnp.where(weight > 0.0, weight, 1.0), 0.0)

    last_row = begin + (cx + 2) * pitch - 3

    own_first, own_last = cx * pitch + 2, (2 * cx - 1) * pitch + 1 + cy

    def pair_values(n, last):
        dx, dy, dz = HALF[n]
        shift = dx * pitch + dy
        for start in range(begin - max(shift, 0), last_row + 1 - min(shift, 0), 8):
            parts = []
            for q, d in enumerate((dx, dy, dz)):
                far = near[dz + 1, q, start + shift:start + shift + 8]
                parts.append(far - (near[1, q, start:start + 8] - d * UNIT))
            square = parts[0] * parts[0] + parts[1] * parts[1] + parts[2] * parts[2]
            inverse = lax.rsqrt(square)
            growth = jnp.exp2(square * inverse * RATE)
            inside = 1.0 - square
            cut = growth * inside
            halves[n, start:start + 8] = cut * inside
            if start + 8 > own_first - max(shift, 0) and start <= own_last - min(shift, 0):
                steep = PULL + inside * inverse
                bonds[n, 0, start:start + 8] = cut * steep
                bonds[n, 1, start:start + 8] = cut * (growth * (steep - PUSH))
                if last:
                    bonds[n, 2, start:start + 8] = cut * cut

    def main_density(t):
        last = t == ITERS - 1
        for n in range(len(HALF)):
            pair_values(n, last)
        for start in range(begin, last_row + 1, 8):
            total = jnp.zeros((8, LANES), f32)
            behind = jnp.zeros((8, LANES), f32)
            for n, (dx, dy, dz) in enumerate(HALF):
                to = start + dx * pitch + dy
                back = start - dx * pitch - dy
                total = total + near[dz + 1, 3, to:to + 8] * halves[n, start:start + 8]
                reaction = near[1, 3, back:back + 8] * halves[n, back:back + 8]
                if dz == 0:
                    total = total + reaction
                else:
                    behind = behind + reaction
            total = 1.0 + SQUARED_E * (total + moved(behind, 1))
            root = lax.rsqrt(total)
            slope = scaled[start:start + 8] * root
            slopes[0, start:start + 8] = moved(slope, 1)
            slopes[1, start:start + 8] = slope
            slopes[2, start:start + 8] = moved(slope, -1)
            if last:
                slopes[3, start:start + 8] = total * root

    def main_force(t, slabs):
        last = t == ITERS - 1
        values = []
        for x in slabs:
            start = (cx + x) * pitch + 2
            here = [mine[q][x] for q in range(3)]
            base = [[h - s * UNIT for s in (-1.0, 0.0, 1.0)] for h in here]
            slope = slopes[1, start:start + cy]
            force = [jnp.zeros((cy, LANES), f32) for _ in range(3)]
            pair = jnp.zeros((cy, LANES), f32)
            for o in AROUND:
                row = start + o[0] * pitch + o[1]

                def bond(k, o=o, row=row):
                    if o in HALF:
                        return bonds[HALF.index(o), k, start:start + cy]
                    return moved(bonds[HALF.index(minus(o)), k, row:row + cy], -o[2])

                far = near[o[2] + 1, 3, row:row + cy]
                scale = far * ((slope + slopes[o[2] + 1, row:row + cy]) * bond(0) + bond(1))
                force = [force[q] + scale * (near[o[2] + 1, q, row:row + cy] - base[q][d + 1])
                         for q, d in enumerate(o)]
                if last:
                    pair = pair + far * bond(2)
            weight = mine[3][x]
            if last:
                values.append([(weight * FORCE) * f for f in force] + [
                    (weight * PAIR) * pair - jnp.where(weight > 0.0, slopes[3, start:start + cy], 0.0)])
            else:
                for q in range(3):
                    mine[q][x] = here[q] + (weight * (FORCE * STEP * UNIT)) * force[q]
        return values

    def main_send_next(t):
        fill_sends(t + 1)
        send(*main_plan(t + 1))
        put_mine(t + 1)

    def merge(values):
        outer = (lane < DEEP) | (lane >= cz - DEEP)
        for x in range(cx):
            start = group + x * wide + DEEP
            for q in range(4):
                spot = force_ref.at[q, x] if q < 3 else energy_ref.at[x]
                spot[...] = jnp.where(outer, moved(final[start:start + cy], cz - 8 - 16 * q), values[x][q])

    def spread(parts, at):
        found = [moved(parts[i], group * (i - at)) for i in range(3)]
        return jnp.where(lane < group, found[0], jnp.where(
            lane < 2 * group, found[1], jnp.where(lane < 3 * group, found[2], 0.0)))

    def put_strip(q, row, value):
        for j, (dx, dy) in enumerate(PLANE):
            sp[j, q, row:row + 8] = moved(value, -(dx * wide + dy))

    def strip_arrive(t):
        if t == 0:
            settle(panel_total, panel_recv)
            settle(panel_total, panel_send)

            def flat(rows):
                return [sum(ps[1, rows:rows + 8] if (dx, dy) == (0, 0)
                            else px[PLANE.index((dx, dy)), rows:rows + 8] for dy in (-1, 0, 1))
                        for dx in (-1, 0, 1)]

            def tall(side, rows):
                return [sum(pz[PLANE.index((dx, dy)), side, rows:rows + 8] for dy in (-1, 0, 1))
                        for dx in (-1, 0, 1)]

            blocks = [tall(0, 8), flat(8), flat(0), flat(24), tall(1, 0)]
            for b, parts in enumerate(blocks):
                for q in range(3):
                    put_strip(q, 8 * b, spread(parts, q))
            loads_at = flat(16)
            for b, (parts, at) in enumerate(((tall(0, 0), 2), (loads_at, 0), (loads_at, 1),
                                             (loads_at, 2), (tall(1, 8), 0))):
                weight = spread(parts, at)
                put_strip(3, 8 * b, weight)
                sscaled[8 * b:8 * b + 8] = jnp.where(
                    weight > 0.0, (-0.5 / SQUARED_E) / jnp.where(weight > 0.0, weight, 1.0), 0.0)
        else:
            settle(64, strip_recv.at[t - 1])
            settle(64, strip_send.at[t - 1])
            for b in range(4):
                for q in range(3):
                    under = moved(xq[t - 1, 0, 8 * b:8 * b + 8], -group * q)
                    over = moved(xq[t - 1, 1, 8 * b:8 * b + 8], group * (2 - q))
                    put_strip(q, 4 + 8 * b, jnp.where(lane < group, under, jnp.where(
                        lane < 2 * group, sn[q, 4 + 8 * b:12 + 8 * b],
                        jnp.where(lane < 3 * group, over, 0.0))))


    def strip_density(t):
        last = t == ITERS - 1
        reach = 2 * (ITERS - 1 - t)
        starts = []
        for base in (8, 32 - DEEP):
            starts += sorted({base - reach - 1, base + DEEP + reach + 1 - 8})
        pairs = []
        for n, row in enumerate(starts):
            def around(dx, dy, dz, q, row=row):
                return sp[PLANE.index((dx, dy)), q, row + dz:row + dz + 8]

            total, pair = density_and_factors(
                around, [sp[4, q, row:row + 8] for q in range(3)], factors.at[n], last)
            total = 1.0 + SQUARED_E * total
            root = lax.rsqrt(total)
            slope = sscaled[row:row + 8] * root
            for j, (dx, dy) in enumerate(PLANE):
                ss[j, row:row + 8] = moved(slope, -(dx * wide + dy))
            weight = sp[4, 3, row:row + 8]
            if last:
                pairs.append((weight * PAIR) * pair - jnp.where(weight > 0.0, total * root, 0.0))
        return starts, pairs

    def strip_force(t, starts, pairs):
        last = t == ITERS - 1
        for n, row in enumerate(starts):
            def around(dx, dy, dz, q, row=row):
                return sp[PLANE.index((dx, dy)), q, row + dz:row + dz + 8]

            def slope_around(dx, dy, dz, row=row):
                return ss[PLANE.index((dx, dy)), row + dz:row + dz + 8]

            here = [sp[4, q, row:row + 8] for q in range(3)]
            force = force_from_factors(around, slope_around, here, ss[4, row:row + 8], factors.at[n])
            weight = sp[4, 3, row:row + 8]
            if last:
                for q, value in enumerate([(weight * FORCE) * f for f in force] + [pairs[n]]):
                    tails[q, n, n:n + 8] = value
            else:
                for q in range(3):
                    sn[q, row:row + 8] = here[q] + (weight * (FORCE * STEP * UNIT)) * force[q]
        if not last:
            for b in range(4):
                new = [moved(sn[q, 4 + 8 * b:12 + 8 * b], group * (q - 1)) for q in range(3)]
                xp[t, 8 * b:8 * b + 8] = jnp.where(
                    lane < group, new[0], jnp.where(lane < 2 * group, new[1], new[2]))
            send(*strip_plan(t))
            return
        rows = []
        for q in range(4):
            rows += [tails[q, 1, 0:8], tails[q, 0, 1:9]]
        rows.append(jnp.zeros((LANES - 64, LANES), f32))
        final[...] = jnp.transpose(jnp.concatenate(rows, axis=0))

    for t in range(ITERS):
        main_arrive(t)
        if t < ITERS - 1:
            main_density(t)
            main_force(t, range(cx))
            main_send_next(t)
            strip_arrive(t)
            strip_force(t, *strip_density(t))
            fill(*strip_plan(t))
            if t + 2 < ITERS:
                fill(*main_plan(t + 2))
        else:
            main_density(t)
            strip_arrive(t)
            strips = strip_density(t)
            values = main_force(t, [0])
            strip_force(t, *strips)
            merge(values + main_force(t, range(1, cx)))


def put_out(force_ref, energy_ref, force_hbm, energy_hbm, sem):
    copies = [pltpu.make_async_copy(force_ref, force_hbm, sem.at[0]),
              pltpu.make_async_copy(energy_ref, energy_hbm, sem.at[1])]
    for copy in copies:
        copy.start()
    for copy in copies:
        copy.wait()


def solution(mesh):
    counts = tuple(mesh.shape[axis] for axis in AXES)

    def body(displace, occupied, strength):
        sizes = occupied.shape
        cx, cy, cz = sizes
        assert cx == 2 and cy == 8 and cz == LANES
        pitch = cy + 4
        rows = up(2 * (pitch + 1) + up((cx + 2) * pitch + cy + 3 - (pitch + 1)))
        f32 = jnp.float32
        vmem = pl.BlockSpec(memory_space=pltpu.VMEM)
        force, energy = pl.pallas_call(
            functools.partial(kernel, sizes, counts),
            out_shape=(pltpu.VMEM((3,) + sizes, f32), pltpu.VMEM(sizes, f32)),
            in_specs=[pl.BlockSpec(memory_space=pl.ANY)] * 3,
            out_specs=(vmem, vmem),
            scratch_shapes=[
                pltpu.VMEM((3,) + sizes, f32),
                pltpu.VMEM(sizes, jnp.int32),
                pltpu.VMEM(sizes, f32),
                pltpu.VMEM((ITERS, 4 * cx * cy, LANES), f32),
                pltpu.VMEM((ITERS, 2, up(8 * cx), LANES), f32),
                pltpu.VMEM((ITERS, 2, 4 * cx * cy, LANES), f32),
                pltpu.VMEM((ITERS, 3, 2, up(8 * cx), LANES), f32),
                pltpu.VMEM((3, 4, rows, LANES), f32),
                pltpu.VMEM((4, rows, LANES), f32),
                pltpu.VMEM((rows, LANES), f32),
                pltpu.VMEM((len(HALF), rows, LANES), f32),
                pltpu.VMEM((len(HALF), 3, rows, LANES), f32),
                pltpu.VMEM((2, LANES, LANES), f32),
                pltpu.VMEM((3, 32, LANES), f32),
                pltpu.VMEM((9, 32, LANES), f32),
                pltpu.VMEM((9, 2, 16, LANES), f32),
                pltpu.VMEM((9, 4, 40, LANES), f32),
                pltpu.VMEM((3, 40, LANES), f32),
                pltpu.VMEM((9, 40, LANES), f32),
                pltpu.VMEM((40, LANES), f32),
                pltpu.VMEM((ITERS - 1, 32, LANES), f32),
                pltpu.VMEM((ITERS - 1, 2, 32, LANES), f32),
                pltpu.VMEM((LANES, LANES), f32),
                pltpu.VMEM((4 * cx * cy, LANES), f32),
                pltpu.VMEM((2, 2, 4 * cx * cy, LANES), f32),
                pltpu.VMEM((2, 3, 2, up(8 * cx), LANES), f32),
                pltpu.VMEM((9, 32, LANES), f32),
                pltpu.VMEM((9, 2, 16, LANES), f32),
                pltpu.VMEM((ITERS - 1, 2, 32, LANES), f32),
                pltpu.VMEM((8 * 32 + 18 * 16, LANES), f32),
                pltpu.VMEM((4, 26, 2, 8, LANES), f32),
                pltpu.VMEM((4, 2, 16, LANES), f32),
                pltpu.SemaphoreType.DMA((2,)),
                pltpu.SemaphoreType.DMA((2,)),
                pltpu.SemaphoreType.DMA,
                pltpu.SemaphoreType.DMA,
                pltpu.SemaphoreType.DMA((ITERS - 1,)),
                pltpu.SemaphoreType.DMA((ITERS - 1,)),
                pltpu.SemaphoreType.DMA,
            ],
            compiler_params=pltpu.CompilerParams(collective_id=0, has_side_effects=True),
        )(displace, occupied, strength)
        return pl.pallas_call(
            put_out,
            out_shape=(jax.ShapeDtypeStruct((3,) + sizes, f32), jax.ShapeDtypeStruct(sizes, f32)),
            in_specs=[vmem, vmem],
            out_specs=(pl.BlockSpec(memory_space=pl.ANY),) * 2,
            scratch_shapes=[pltpu.SemaphoreType.DMA((2,))],
        )(pltpu.with_memory_space_constraint(force, pltpu.VMEM),
          pltpu.with_memory_space_constraint(energy, pltpu.VMEM))

    in_specs = (P(None, "gx", "gy", "gz"), P("gx", "gy", "gz"), P("gx", "gy", "gz"))
    out_specs = (P(None, "gx", "gy", "gz"), P("gx", "gy", "gz"))
    return jax.shard_map(body, mesh=mesh, in_specs=in_specs, out_specs=out_specs, check_vma=False)
```

```python
import functools
import math

import jax
import jax.numpy as jnp
from jax import lax
from jax.experimental import pallas as pl
from jax.experimental.pallas import tpu as pltpu
from jax.sharding import PartitionSpec as P

ITERS = 3
RADIUS_SQ = 4.84
STEP = 0.02
AXES = ("gx", "gy", "gz")
MESH = pl.DeviceIdType.MESH
LANES = 128
DEEP = 2 * ITERS
PLANE = [(dx, dy) for dx in (-1, 0, 1) for dy in (-1, 0, 1)]
FLAT = sorted(((dx, dy, 0) for dx, dy in PLANE if (dx, dy) != (0, 0)),
              key=lambda o: (-abs(o[1]), abs(o[0]), o))
TALL = sorted(((dx, dy, dz) for dx, dy in PLANE for dz in (-1, 1)),
              key=lambda o: (-sum(abs(a) for a in o), o))
PANELS = TALL + FLAT
HALF = [(dx, dy, 1) for dx, dy in PLANE] + [(1, -1, 0), (1, 0, 0), (1, 1, 0), (0, 1, 0)]
AROUND = [(dx, dy, dz) for dx, dy in PLANE for dz in (-1, 0, 1) if (dx, dy, dz) != (0, 0, 0)]
SIDES = [(-1, 0, 0), (1, 0, 0)]

RADIUS = math.sqrt(RADIUS_SQ)
UNIT = 1.0 / RADIUS
RATE = -2.0 * RADIUS / math.log(2.0)
SQUARED_E = math.exp(2.0)
PULL = 2.0 / RADIUS
PUSH = 1.0 / RADIUS
FORCE = -2.0 * SQUARED_E * SQUARED_E
PAIR = 0.5 * 0.5 * SQUARED_E * SQUARED_E


def minus(o):
    return tuple(-a for a in o)


def up(rows):
    return -(-rows // 8) * 8


def low(a):
    return 0 if a == -1 else 1


def moved(value, amount, axis=1):
    amount %= value.shape[axis]
    return value if amount == 0 else pltpu.roll(value, amount, axis)


def density_and_factors(near, here, factors, last):
    base = [[h - s * UNIT for s in (-1.0, 0.0, 1.0)] for h in here]
    total = jnp.zeros((8, LANES), jnp.float32)
    pair = jnp.zeros((8, LANES), jnp.float32)
    for n, (dx, dy, dz) in enumerate(AROUND):
        sx = near(dx, dy, dz, 0) - base[0][dx + 1]
        sy = near(dx, dy, dz, 1) - base[1][dy + 1]
        sz = near(dx, dy, dz, 2) - base[2][dz + 1]
        square = sx * sx + sy * sy + sz * sz
        inverse = lax.rsqrt(square)
        growth = jnp.exp2(square * inverse * RATE)
        inside = 1.0 - square
        steep = PULL + inside * inverse
        cut = growth * inside
        heavy = cut * near(dx, dy, dz, 3)
        total = total + heavy * inside
        factors[n, 0] = heavy * steep
        factors[n, 1] = heavy * (growth * (steep - PUSH))
        if last:
            pair = pair + heavy * cut
    return total, pair


def force_from_factors(near, slope_near, here, slope, factors):
    base = [[h - s * UNIT for s in (-1.0, 0.0, 1.0)] for h in here]
    force = [jnp.zeros((8, LANES), jnp.float32) for _ in range(3)]
    for n, (dx, dy, dz) in enumerate(AROUND):
        scale = (slope + slope_near(dx, dy, dz)) * factors[n, 0] + factors[n, 1]
        force = [force[q] + scale * (near(dx, dy, dz, q) - base[q][d + 1])
                 for q, d in enumerate((dx, dy, dz))]
    return force


def kernel(sizes, counts, disp_hbm, occ_hbm, str_hbm, force_ref, energy_ref,
           disp_ref, occ_ref, str_ref, xs, ys, xl, yl, near, slopes, scaled, halves, bonds,
           stage, ps, px, pz, sp, sn, ss, sscaled, xp, xq, final,
           zero, sink_xl, sink_yl, sink_px, sink_pz, sink_xq, tally, factors, tails,
           main_send, main_recv, panel_send, panel_recv, strip_send, strip_recv, load_sem):
    cx, cy, cz = sizes
    pitch = cy + 4
    wide = cy + 2 * DEEP
    group = cx * wide
    f32 = jnp.float32

    for src, dst in ((disp_hbm, disp_ref), (occ_hbm, occ_ref), (str_hbm, str_ref)):
        pltpu.make_async_copy(src, dst, load_sem).start()
    zero[...] = jnp.zeros(zero.shape, f32)

    def settle(rows, sem):
        part = tally.at[pl.ds(0, rows)]
        pltpu.make_async_copy(part, part, sem).wait()

    me = [lax.axis_index(axis) for axis in AXES]
    there = [[None if s == 0 else (m + s >= 0) & (m + s < n) for s in (-1, 0, 1)]
             for m, n in zip(me, counts)]

    def exists(o):
        tests = [there[a][o[a] + 1] for a in range(3) if o[a] != 0]
        return functools.reduce(lambda p, q: p & q, tests)

    def target(o):
        return {AXES[a]: me[a] + o[a] for a in range(3)}

    barrier = pltpu.get_barrier_semaphore()
    for o in PANELS:
        @pl.when(exists(o))
        def _(o=o):
            pl.semaphore_signal(barrier, inc=1, device_id=target(o), device_id_type=MESH)
    spans = [1 + (m > 0).astype(jnp.int32) + (m < n - 1).astype(jnp.int32)
             for m, n in zip(me, counts)]

    def main_rows(t, face):
        return (4 if t == 0 else 3) * cx * (cy if face else 2)

    def send(plan, send_sem, recv_sem):
        for o, src, spot, _ in plan:
            @pl.when(exists(o))
            def _(o=o, src=src, spot=spot):
                pltpu.make_async_remote_copy(
                    src_ref=src, dst_ref=spot(minus(o)), send_sem=send_sem, recv_sem=recv_sem,
                    device_id=target(o), device_id_type=MESH).start()

    def fill(plan, send_sem, recv_sem):
        for o, src, spot, sink in plan:
            @pl.when(jnp.logical_not(exists(o)))
            def _(o=o, src=src, spot=spot, sink=sink):
                blank = zero.at[pl.ds(0, src.shape[0])]
                pltpu.make_async_copy(blank, spot(o), recv_sem).start()
                pltpu.make_async_copy(blank, sink(o), send_sem).start()

    def main_plan(t):
        plan = []
        for o in FLAT:
            rows = pl.ds(0, main_rows(t, o[1] == 0))
            if o[1] == 0:
                plan.append((o, xs.at[t, rows], lambda n, r=rows: xl.at[t, low(n[0]), r],
                             lambda n, r=rows: sink_xl.at[t % 2, low(n[0]), r]))
            else:
                plan.append((o, ys.at[t, low(-o[1]), rows],
                             lambda n, r=rows: yl.at[t, n[0] + 1, low(n[1]), r],
                             lambda n, r=rows: sink_yl.at[t % 2, n[0] + 1, low(n[1]), r]))
        return plan, main_send.at[t % 2], main_recv.at[t % 2]

    def main_total(t):
        return 2 * main_rows(t, True) + 6 * main_rows(t, False)

    def panel_plan():
        plan = []
        for o in PANELS:
            if o[2] == 0:
                plan.append((o, ps.at[1 - o[1], pl.ds(0, 32)],
                             lambda n: px.at[PLANE.index(n[:2])],
                             lambda n: sink_px.at[PLANE.index(n[:2])]))
            else:
                plan.append((o, ps.at[1 - o[1], pl.ds(8 if o[2] == -1 else 16, 16)],
                             lambda n: pz.at[PLANE.index(n[:2]), low(n[2])],
                             lambda n: sink_pz.at[PLANE.index(n[:2]), low(n[2])]))
        return plan, panel_send, panel_recv

    panel_total = 8 * 32 + 18 * 16

    def strip_plan(t):
        plan = [(o, xp.at[t], lambda n: xq.at[t, low(n[0])], lambda n: sink_xq.at[t, low(n[0])])
                for o in SIDES]
        return plan, strip_send.at[t], strip_recv.at[t]


    settle(5 * cx * cy, load_sem)
    mine = [[disp_ref[q, x] * UNIT for x in range(cx)] for q in range(3)]
    mine.append([occ_ref[x].astype(f32) * str_ref[x] for x in range(cx)])

    def fill_sends(t):
        for q in range(4 if t == 0 else 3):
            for x in range(cx):
                i = q * cx + x
                xs[t, i * cy:(i + 1) * cy] = mine[q][x]
                ys[t, 0, i * 2:i * 2 + 2] = mine[q][x][cy - 2:cy]
                ys[t, 1, i * 2:i * 2 + 2] = mine[q][x][0:2]

    def put(q, row, piece):
        rows = piece.shape[0]
        near[0, q, row:row + rows] = moved(piece, 1)
        near[1, q, row:row + rows] = piece
        near[2, q, row:row + rows] = moved(piece, -1)

    def put_mine(t):
        for q in range(4 if t == 0 else 3):
            for x in range(cx):
                put(q, (cx + x) * pitch + 2, mine[q][x])

    def put_others(t):
        for q in range(4 if t == 0 else 3):
            for x in range(cx):
                i = q * cx + x
                for dx in (-1, 0, 1):
                    row = (cx * (dx + 1) + x) * pitch
                    if dx != 0:
                        put(q, row + 2, xl[t, low(dx), i * cy:(i + 1) * cy])
                    put(q, row, yl[t, dx + 1, 0, i * 2:i * 2 + 2])
                    put(q, row + 2 + cy, yl[t, dx + 1, 1, i * 2:i * 2 + 2])

    fill_sends(0)
    stage[...] = jnp.zeros(stage.shape, f32)

    lane = lax.broadcasted_iota(jnp.int32, (8, LANES), 1)
    half = lax.broadcasted_iota(jnp.int32, (8, LANES), 0) < 4
    column = lax.rem(lane, wide)
    for x in range(cx):
        for q in range(3):
            row = q * group + x * wide + DEEP
            stage[0, row:row + cy] = mine[q][x]
            stage[1, row:row + cy] = mine[3][x]
    turned = jnp.transpose(stage[0])
    heavy = jnp.transpose(stage[1])

    def ends_of(value):
        return (value[0:8], jnp.where(half, value[8:16], value[cz - 16:cz - 8]), value[cz - 8:cz])

    first, middle, end = ends_of(turned)
    load_first, load_middle, load_end = ends_of(heavy)
    load = jnp.where(lane < group, load_first, jnp.where(lane < 2 * group, load_middle, load_end))
    for i, piece in enumerate((middle, first, load, end)):
        ps[1, 8 * i:8 * i + 8] = piece
        ps[0, 8 * i:8 * i + 8] = jnp.where(column < DEEP, moved(piece, -cy), 0.0)
        ps[2, 8 * i:8 * i + 8] = jnp.where(column >= DEEP + cy, moved(piece, cy), 0.0)
    pl.semaphore_wait(barrier, spans[0] * spans[1] * spans[2] - 1)
    send(*main_plan(0))
    send(*panel_plan())
    fill(*main_plan(0))
    fill(*panel_plan())
    tails[...] = jnp.zeros(tails.shape, f32)
    tail = 3 * cx * pitch
    near[:, :, tail:] = jnp.zeros(near.shape[:2] + (near.shape[2] - tail, LANES), f32)
    sn[...] = jnp.zeros(sn.shape, f32)
    ss[...] = jnp.zeros(ss.shape, f32)
    put_mine(0)
    fill(*main_plan(1))

    begin = pitch + 1
    extent = up((cx + 2) * pitch + cy + 3 - begin)

    def main_arrive(t):
        settle(main_total(t), main_recv.at[t % 2])
        settle(main_total(t), main_send.at[t % 2])
        put_others(t)
        if t == 0:
            weight = near[1, 3, begin:begin + extent]
            scaled[begin:begin + extent] = jnp.where(
                weight > 0.0, (-0.5 / SQUARED_E) / jnp.where(weight > 0.0, weight, 1.0), 0.0)

    last_row = begin + (cx + 2) * pitch - 3

    own_first, own_last = cx * pitch + 2, (2 * cx - 1) * pitch + 1 + cy

    def pair_values(n, last):
        dx, dy, dz = HALF[n]
        shift = dx * pitch + dy
        for start in range(begin - max(shift, 0), last_row + 1 - min(shift, 0), 8):
            parts = []
            for q, d in enumerate((dx, dy, dz)):
                far = near[dz + 1, q, start + shift:start + shift + 8]
                parts.append(far - (near[1, q, start:start + 8] - d * UNIT))
            square = parts[0] * parts[0] + parts[1] * parts[1] + parts[2] * parts[2]
            inverse = lax.rsqrt(square)
            growth = jnp.exp2(square * inverse * RATE)
            inside = 1.0 - square
            cut = growth * inside
            halves[n, start:start + 8] = cut * inside
            if start + 8 > own_first - max(shift, 0) and start <= own_last - min(shift, 0):
                steep = PULL + inside * inverse
                bonds[n, 0, start:start + 8] = cut * steep
                bonds[n, 1, start:start + 8] = cut * (growth * (steep - PUSH))
                if last:
                    bonds[n, 2, start:start + 8] = cut * cut

    def main_density(t):
        last = t == ITERS - 1
        for n in range(len(HALF)):
            pair_values(n, last)
        for start in range(begin, last_row + 1, 8):
            total = jnp.zeros((8, LANES), f32)
            behind = jnp.zeros((8, LANES), f32)
            for n, (dx, dy, dz) in enumerate(HALF):
                to = start + dx * pitch + dy
                back = start - dx * pitch - dy
                total = total + near[dz + 1, 3, to:to + 8] * halves[n, start:start + 8]
                reaction = near[1, 3, back:back + 8] * halves[n, back:back + 8]
                if dz == 0:
                    total = total + reaction
                else:
                    behind = behind + reaction
            total = 1.0 + SQUARED_E * (total + moved(behind, 1))
            root = lax.rsqrt(total)
            slope = scaled[start:start + 8] * root
            slopes[0, start:start + 8] = moved(slope, 1)
            slopes[1, start:start + 8] = slope
            slopes[2, start:start + 8] = moved(slope, -1)
            if last:
                slopes[3, start:start + 8] = total * root

    def main_force(t):
        last = t == ITERS - 1
        for x in range(cx):
            start = (cx + x) * pitch + 2
            here = [mine[q][x] for q in range(3)]
            base = [[h - s * UNIT for s in (-1.0, 0.0, 1.0)] for h in here]
            slope = slopes[1, start:start + cy]
            force = [jnp.zeros((cy, LANES), f32) for _ in range(3)]
            pair = jnp.zeros((cy, LANES), f32)
            for o in AROUND:
                row = start + o[0] * pitch + o[1]

                def bond(k, o=o, row=row):
                    if o in HALF:
                        return bonds[HALF.index(o), k, start:start + cy]
                    return moved(bonds[HALF.index(minus(o)), k, row:row + cy], -o[2])

                far = near[o[2] + 1, 3, row:row + cy]
                scale = far * ((slope + slopes[o[2] + 1, row:row + cy]) * bond(0) + bond(1))
                force = [force[q] + scale * (near[o[2] + 1, q, row:row + cy] - base[q][d + 1])
                         for q, d in enumerate(o)]
                if last:
                    pair = pair + far * bond(2)
            weight = mine[3][x]
            if last:
                for q in range(3):
                    force_ref[q, x] = (weight * FORCE) * force[q]
                energy_ref[x] = (weight * PAIR) * pair - jnp.where(
                    weight > 0.0, slopes[3, start:start + cy], 0.0)
            else:
                for q in range(3):
                    mine[q][x] = here[q] + (weight * (FORCE * STEP * UNIT)) * force[q]

    def main_send_next(t):
        fill_sends(t + 1)
        send(*main_plan(t + 1))
        put_mine(t + 1)

    def merge():
        outer = (lane < DEEP) | (lane >= cz - DEEP)
        for x in range(cx):
            start = group + x * wide + DEEP
            for q in range(4):
                spot = force_ref.at[q, x] if q < 3 else energy_ref.at[x]
                spot[...] = jnp.where(outer, moved(final[start:start + cy], cz - 8 - 16 * q), spot[...])

    def spread(parts, at):
        found = [moved(parts[i], group * (i - at)) for i in range(3)]
        return jnp.where(lane < group, found[0], jnp.where(
            lane < 2 * group, found[1], jnp.where(lane < 3 * group, found[2], 0.0)))

    def put_strip(q, row, value):
        for j, (dx, dy) in enumerate(PLANE):
            sp[j, q, row:row + 8] = moved(value, -(dx * wide + dy))

    def strip_arrive(t):
        if t == 0:
            settle(panel_total, panel_recv)
            settle(panel_total, panel_send)

            def flat(rows):
                return [sum(ps[1, rows:rows + 8] if (dx, dy) == (0, 0)
                            else px[PLANE.index((dx, dy)), rows:rows + 8] for dy in (-1, 0, 1))
                        for dx in (-1, 0, 1)]

            def tall(side, rows):
                return [sum(pz[PLANE.index((dx, dy)), side, rows:rows + 8] for dy in (-1, 0, 1))
                        for dx in (-1, 0, 1)]

            blocks = [tall(0, 8), flat(8), flat(0), flat(24), tall(1, 0)]
            for b, parts in enumerate(blocks):
                for q in range(3):
                    put_strip(q, 8 * b, spread(parts, q))
            loads_at = flat(16)
            for b, (parts, at) in enumerate(((tall(0, 0), 2), (loads_at, 0), (loads_at, 1),
                                             (loads_at, 2), (tall(1, 8), 0))):
                weight = spread(parts, at)
                put_strip(3, 8 * b, weight)
                sscaled[8 * b:8 * b + 8] = jnp.where(
                    weight > 0.0, (-0.5 / SQUARED_E) / jnp.where(weight > 0.0, weight, 1.0), 0.0)
        else:
            settle(64, strip_recv.at[t - 1])
            settle(64, strip_send.at[t - 1])
            for b in range(4):
                for q in range(3):
                    under = moved(xq[t - 1, 0, 8 * b:8 * b + 8], -group * q)
                    over = moved(xq[t - 1, 1, 8 * b:8 * b + 8], group * (2 - q))
                    put_strip(q, 4 + 8 * b, jnp.where(lane < group, under, jnp.where(
                        lane < 2 * group, sn[q, 4 + 8 * b:12 + 8 * b],
                        jnp.where(lane < 3 * group, over, 0.0))))


    def strip_density(t):
        last = t == ITERS - 1
        reach = 2 * (ITERS - 1 - t)
        starts = []
        for base in (8, 32 - DEEP):
            starts += sorted({base - reach - 1, base + DEEP + reach + 1 - 8})
        pairs = []
        for n, row in enumerate(starts):
            def around(dx, dy, dz, q, row=row):
                return sp[PLANE.index((dx, dy)), q, row + dz:row + dz + 8]

            total, pair = density_and_factors(
                around, [sp[4, q, row:row + 8] for q in range(3)], factors.at[n], last)
            total = 1.0 + SQUARED_E * total
            root = lax.rsqrt(total)
            slope = sscaled[row:row + 8] * root
            for j, (dx, dy) in enumerate(PLANE):
                ss[j, row:row + 8] = moved(slope, -(dx * wide + dy))
            weight = sp[4, 3, row:row + 8]
            if last:
                pairs.append((weight * PAIR) * pair - jnp.where(weight > 0.0, total * root, 0.0))
        return starts, pairs

    def strip_force(t, starts, pairs):
        last = t == ITERS - 1
        for n, row in enumerate(starts):
            def around(dx, dy, dz, q, row=row):
                return sp[PLANE.index((dx, dy)), q, row + dz:row + dz + 8]

            def slope_around(dx, dy, dz, row=row):
                return ss[PLANE.index((dx, dy)), row + dz:row + dz + 8]

            here = [sp[4, q, row:row + 8] for q in range(3)]
            force = force_from_factors(around, slope_around, here, ss[4, row:row + 8], factors.at[n])
            weight = sp[4, 3, row:row + 8]
            if last:
                for q, value in enumerate([(weight * FORCE) * f for f in force] + [pairs[n]]):
                    tails[q, n, n:n + 8] = value
            else:
                for q in range(3):
                    sn[q, row:row + 8] = here[q] + (weight * (FORCE * STEP * UNIT)) * force[q]
        if not last:
            for b in range(4):
                new = [moved(sn[q, 4 + 8 * b:12 + 8 * b], group * (q - 1)) for q in range(3)]
                xp[t, 8 * b:8 * b + 8] = jnp.where(
                    lane < group, new[0], jnp.where(lane < 2 * group, new[1], new[2]))
            send(*strip_plan(t))
            return
        rows = []
        for q in range(4):
            rows += [tails[q, 1, 0:8], tails[q, 0, 1:9]]
        rows.append(jnp.zeros((LANES - 64, LANES), f32))
        final[...] = jnp.transpose(jnp.concatenate(rows, axis=0))

    for t in range(ITERS):
        main_arrive(t)
        if t < ITERS - 1:
            main_density(t)
            main_force(t)
            main_send_next(t)
            strip_arrive(t)
            strip_force(t, *strip_density(t))
            fill(*strip_plan(t))
            if t + 2 < ITERS:
                fill(*main_plan(t + 2))
        else:
            main_density(t)
            main_force(t)
            strip_arrive(t)
            strip_force(t, *strip_density(t))
            merge()


def put_out(force_ref, energy_ref, force_hbm, energy_hbm, sem):
    copies = [pltpu.make_async_copy(force_ref, force_hbm, sem.at[0]),
              pltpu.make_async_copy(energy_ref, energy_hbm, sem.at[1])]
    for copy in copies:
        copy.start()
    for copy in copies:
        copy.wait()


def solution(mesh):
    counts = tuple(mesh.shape[axis] for axis in AXES)

    def body(displace, occupied, strength):
        sizes = occupied.shape
        cx, cy, cz = sizes
        assert cx == 2 and cy == 8 and cz == LANES
        pitch = cy + 4
        rows = up(2 * (pitch + 1) + up((cx + 2) * pitch + cy + 3 - (pitch + 1)))
        f32 = jnp.float32
        vmem = pl.BlockSpec(memory_space=pltpu.VMEM)
        force, energy = pl.pallas_call(
            functools.partial(kernel, sizes, counts),
            out_shape=(pltpu.VMEM((3,) + sizes, f32), pltpu.VMEM(sizes, f32)),
            in_specs=[pl.BlockSpec(memory_space=pl.ANY)] * 3,
            out_specs=(vmem, vmem),
            scratch_shapes=[
                pltpu.VMEM((3,) + sizes, f32),
                pltpu.VMEM(sizes, jnp.int32),
                pltpu.VMEM(sizes, f32),
                pltpu.VMEM((ITERS, 4 * cx * cy, LANES), f32),
                pltpu.VMEM((ITERS, 2, up(8 * cx), LANES), f32),
                pltpu.VMEM((ITERS, 2, 4 * cx * cy, LANES), f32),
                pltpu.VMEM((ITERS, 3, 2, up(8 * cx), LANES), f32),
                pltpu.VMEM((3, 4, rows, LANES), f32),
                pltpu.VMEM((4, rows, LANES), f32),
                pltpu.VMEM((rows, LANES), f32),
                pltpu.VMEM((len(HALF), rows, LANES), f32),
                pltpu.VMEM((len(HALF), 3, rows, LANES), f32),
                pltpu.VMEM((2, LANES, LANES), f32),
                pltpu.VMEM((3, 32, LANES), f32),
                pltpu.VMEM((9, 32, LANES), f32),
                pltpu.VMEM((9, 2, 16, LANES), f32),
                pltpu.VMEM((9, 4, 40, LANES), f32),
                pltpu.VMEM((3, 40, LANES), f32),
                pltpu.VMEM((9, 40, LANES), f32),
                pltpu.VMEM((40, LANES), f32),
                pltpu.VMEM((ITERS - 1, 32, LANES), f32),
                pltpu.VMEM((ITERS - 1, 2, 32, LANES), f32),
                pltpu.VMEM((LANES, LANES), f32),
                pltpu.VMEM((4 * cx * cy, LANES), f32),
                pltpu.VMEM((2, 2, 4 * cx * cy, LANES), f32),
                pltpu.VMEM((2, 3, 2, up(8 * cx), LANES), f32),
                pltpu.VMEM((9, 32, LANES), f32),
                pltpu.VMEM((9, 2, 16, LANES), f32),
                pltpu.VMEM((ITERS - 1, 2, 32, LANES), f32),
                pltpu.VMEM((8 * 32 + 18 * 16, LANES), f32),
                pltpu.VMEM((4, 26, 2, 8, LANES), f32),
                pltpu.VMEM((4, 2, 16, LANES), f32),
                pltpu.SemaphoreType.DMA((2,)),
                pltpu.SemaphoreType.DMA((2,)),
                pltpu.SemaphoreType.DMA,
                pltpu.SemaphoreType.DMA,
                pltpu.SemaphoreType.DMA((ITERS - 1,)),
                pltpu.SemaphoreType.DMA((ITERS - 1,)),
                pltpu.SemaphoreType.DMA,
            ],
            compiler_params=pltpu.CompilerParams(collective_id=0, has_side_effects=True),
        )(displace, occupied, strength)
        return pl.pallas_call(
            put_out,
            out_shape=(jax.ShapeDtypeStruct((3,) + sizes, f32), jax.ShapeDtypeStruct(sizes, f32)),
            in_specs=[vmem, vmem],
            out_specs=(pl.BlockSpec(memory_space=pl.ANY),) * 2,
            scratch_shapes=[pltpu.SemaphoreType.DMA((2,))],
        )(pltpu.with_memory_space_constraint(force, pltpu.VMEM),
          pltpu.with_memory_space_constraint(energy, pltpu.VMEM))

    in_specs = (P(None, "gx", "gy", "gz"), P("gx", "gy", "gz"), P("gx", "gy", "gz"))
    out_specs = (P(None, "gx", "gy", "gz"), P("gx", "gy", "gz"))
    return jax.shard_map(body, mesh=mesh, in_specs=in_specs, out_specs=out_specs, check_vma=False)
```
